256 devices in a mesh: groups: 2 (over z), expert: 64 (over x, y), replica: 2 (over core).
Axes of the slice: x: 8, y: 8, z: 2, core: 2. Of those that a mesh axis runs over, the one named last changes fastest.
The devices are a block of a 8x8x16 slice.
Arguments:
- queries: bfloat16 [1024, 8192], P(('groups', 'expert', 'replica')), parts along dimension 0, may hold values from -250 to 250
- token_keys: bfloat16 [1024, 512], P(('groups', 'expert', 'replica')), parts along dimension 0, may hold values from -6 to 6
- token_values: bfloat16 [1024, 512], P(('groups', 'expert', 'replica')), parts along dimension 0, may hold values from -6 to 6
- stored_keys: bfloat16 [1024, 256, 512], P(('groups', 'expert', 'replica')), parts along dimension 0, may hold values from -7 to 7
- stored_values: bfloat16 [1024, 256, 512], P(('groups', 'expert', 'replica')), parts along dimension 0, may hold values from -6 to 6
- kv_len: int32 [1024], P(('groups', 'expert', 'replica')), parts along dimension 0, may hold values from 2 to 256, as said below
- residual: bfloat16 [1024, 4096], P(('groups', 'expert', 'replica')), parts along dimension 0, may hold values from -6 to 6
- out_weight: bfloat16 [8192, 4096], P(('expert', 'replica')), may hold values from -0.1875 to 0.1875
- norm_gain: bfloat16 [4096], replicated, may hold values from 0.25 to 1.75
- expert_ids: int32 [1024, 8], P(('groups', 'expert')), parts along dimension 0, may hold values from 0 to 63, all different within a row; in each aligned block of 8 rows (0 to 7, 8 to 15, ...) at most 2 rows name the same one
- route_weight: float32 [1024, 8], P(('groups', 'expert')), parts along dimension 0, may hold values from 0.05 to 1
- w_gate: bfloat16 [64, 4096, 768], P('expert', None, 'replica'), may hold values from -0.09375 to 0.09375
- w_up: bfloat16 [64, 4096, 768], P('expert', None, 'replica'), may hold values from -0.09375 to 0.09375
- w_down: bfloat16 [64, 768, 4096], P('expert', 'replica'), may hold values from -0.4375 to 0.4375
Outputs:
- updated: bfloat16 [1024, 4096], P(('groups', 'expert', 'replica')), parts along dimension 0
The draws below stay inside these ranges and needn't reach their ends.
There are 2 independent parts, one for each index of `groups`. The reference program is written for one: setup_inputs(seed, part) draws one part's arguments, and reference() takes and returns one part's arrays. A program takes and returns all parts, laid end to end along the dimension named above; an argument that names none is the same for every part. Nothing has to cross between parts.
Inputs may be any that keep to these rules, and one draw needn't show every extreme that they name: `kv_len`: at least 2; some sequence uses all 256 positions. `expert_ids`: each token names 8 different experts; in each aligned block of 8 tokens no expert is named by more than 2 tokens, and some block reaches it.
All inputs are finite; a program needn't handle non-finite values.
Results may differ from the reference program's by a relative error of at most 0.01.
Values may be sent and summed in bfloat16 or wider, within the bound.
A program may use at most 64 MiB of HBM per device.

```python
import math
import jax
import jax.numpy as jnp
import numpy as np
from jax import lax

D = 4096
QUERY_HEADS = 64
KEY_VALUE_HEADS = 4
HEAD_WIDTH = 128
FF = 768
TOPK = 8
SEQ_DEV = 4
CACHE_POSITIONS = 256
EXPERTS = 64
SEQUENCE_TOTAL = 512
MOST = 2
N_EXPERT = 64
N_REPLICA = 2


def key_lookup(key):
    return jnp.clip(jax.random.normal(jax.random.fold_in(key, 11), (SEQUENCE_TOTAL, CACHE_POSITIONS, KEY_VALUE_HEADS * HEAD_WIDTH), jnp.float32), -6.0, 6.0)


def draw_queries(key, part):
    base = jnp.clip(jax.random.normal(jax.random.fold_in(key, 5), (SEQUENCE_TOTAL, QUERY_HEADS * HEAD_WIDTH), jnp.float32), -6.0, 6.0)
    return base.astype(jnp.bfloat16)


def draw_stored_keys(key, part):
    table = key_lookup(key)
    return table.astype(jnp.bfloat16)


def draw_kv_len(key, part):
    lengths = jax.random.randint(jax.random.fold_in(key, 3), (SEQUENCE_TOTAL,), 2, CACHE_POSITIONS + 1, jnp.int32)
    chosen = jax.random.randint(jax.random.fold_in(key, 4), (), 0, SEQUENCE_TOTAL, jnp.int32)
    return jnp.where(jnp.arange(SEQUENCE_TOTAL, dtype=jnp.int32) == chosen, CACHE_POSITIONS, lengths).astype(jnp.int32)


def shard_levels(own_key, shape, cuts, least, high):
    gain, own = 1.0, jax.random.fold_in(own_key, 6)
    for dim, parts in cuts:
        heights = jnp.exp(jax.random.uniform(jax.random.fold_in(own, dim), (parts,), jnp.float32, least / len(cuts), high / len(cuts)))
        gain = gain * jnp.repeat(heights, shape[dim] // parts).reshape([-1 if axis == dim else 1 for axis in range(len(shape))])
    return gain


def shared_out(own_key, own, number, rows, number_of, top, most, slope):
    ranking = jax.random.permutation(own_key, number_of)
    heavy_load, common = portions_of(number_of, rows * top, most, slope, True), portions_of(number_of, rows * top, most, slope, False)
    places = jnp.arange(number_of)

    def named(tallies, turn):
        used = int((tallies > 0).sum())
        fixed = max(1, used // 4)
        shifted = fixed + (places - fixed + turn * (used - fixed)) % max(1, number_of - fixed)
        return jnp.zeros((number_of,), jnp.int32).at[ranking[jnp.where(places < fixed, places, shifted)]].set(jnp.asarray(tallies, jnp.int32))

    tallies = jnp.where(number % 4 == 0, named(heavy_load, number // 4), named(common, number - number // 4 - 1))
    mixed = jax.random.permutation(jax.random.fold_in(own, 3), number_of)
    donor, receiver = mixed[0:number_of // 2 * 2:2], mixed[1:number_of // 2 * 2:2]
    margin = jnp.minimum(tallies[donor] - 1, most - tallies[receiver]) // 2
    margin = jnp.where((donor == ranking[0]) | (receiver == ranking[0]) | (tallies[receiver] == 0), 0, jnp.maximum(margin, 0))
    shifted = jax.random.randint(jax.random.fold_in(own, 4), (number_of // 2,), 0, 1 << 20) % (margin + 1)
    tallies = tallies.at[donor].add(-shifted).at[receiver].add(shifted)
    items = jnp.searchsorted(jnp.cumsum(tallies), jnp.arange(rows * top), side="right").astype(jnp.int32)
    listing = items.reshape(top, rows).T
    listing = listing[jax.random.permutation(jax.random.fold_in(own, 1), rows)]
    turn = jax.random.randint(jax.random.fold_in(own, 2), (rows, 1), 0, top)
    return jnp.take_along_axis(listing, (jnp.arange(top)[None, :] + turn) % top, axis=1)


def portions_of(number_of, total, limit, lean, full):
    portions = [(1 << 20) // math.isqrt(grade ** lean) + 1 for grade in range(1, number_of + 1)]
    largest = limit if full else min(limit, max(-(-total // number_of), total * portions[0] // sum(portions)))
    least = 1 if total - largest >= number_of - 1 else 0
    given, rest = [largest] + [least] * (number_of - 1), total - largest - least * (number_of - 1)
    while rest > 0:
        movable = [i for i in range(1, number_of) if given[i] < largest] or [i for i in range(1, number_of) if given[i] < limit]
        whole, remaining = sum([portions[i] for i in movable]), rest
        for i in movable:
            addition = min(limit - given[i], max(1, remaining * portions[i] // whole), rest)
            given[i] = given[i] + addition
            rest = rest - addition
    return np.array(given)


def normal_values(key, shape, width, reach, pieces=(), held_as=jnp.bfloat16):
    entries = width * jax.random.normal(key, shape, jnp.float32)
    if pieces:
        entries = entries * shard_levels(key, shape, pieces, -0.22, 0.18)
    return jnp.clip(entries, -reach, reach).astype(held_as)


def setup_inputs(seed: int = 0, part: int = 0) -> dict:
    key_list = jax.random.split(jax.random.key(seed), 15)
    part_splits = jax.random.split(jax.random.fold_in(key_list[14], part), 15)
    queries = draw_queries(jax.random.fold_in(jax.random.fold_in(key_list[14], part), 71), part)
    token_keys = normal_values(part_splits[1], (SEQUENCE_TOTAL, KEY_VALUE_HEADS * HEAD_WIDTH), 1.0, 6.0, ((0, 128),))
    token_values = normal_values(part_splits[2], (SEQUENCE_TOTAL, KEY_VALUE_HEADS * HEAD_WIDTH), 1.0, 6.0, ((0, 128),))
    stored_keys = draw_stored_keys(jax.random.fold_in(jax.random.fold_in(key_list[14], part), 71), part)
    stored_values = normal_values(part_splits[4], (SEQUENCE_TOTAL, CACHE_POSITIONS, KEY_VALUE_HEADS * HEAD_WIDTH), 1.0, 6.0, ((0, 128),))
    kv_len = draw_kv_len(jax.random.fold_in(jax.random.fold_in(key_list[14], part), 71), part)
    residual = normal_values(part_splits[6], (SEQUENCE_TOTAL, D), 1.0, 6.0, ((0, 128),))
    out_weight = normal_values(key_list[7], (QUERY_HEADS * HEAD_WIDTH, D), (QUERY_HEADS * HEAD_WIDTH // 8) ** -0.5, 0.1875, ((0, 128),))
    norm_gain = jnp.clip(1.0 + 0.15 * jax.random.normal(key_list[8], (D,), jnp.float32), 0.25, 1.75).astype(jnp.bfloat16)
    expert_ids_keys = jax.random.split(jax.random.fold_in(part_splits[9], 1), SEQUENCE_TOTAL // (N_REPLICA * SEQ_DEV))
    expert_ids_turns = jax.random.permutation(jax.random.fold_in(part_splits[9], 3), SEQUENCE_TOTAL // (N_REPLICA * SEQ_DEV))
    expert_ids = jax.vmap(lambda own, number: shared_out(jax.random.fold_in(part_splits[9], 2), own, number, N_REPLICA * SEQ_DEV, EXPERTS, TOPK, MOST, 2))(expert_ids_keys, expert_ids_turns).reshape((SEQUENCE_TOTAL, TOPK))
    route_weight = jnp.clip(jnp.exp(math.log(1.0) - 2.9957323 * jax.random.uniform(part_splits[10], (SEQUENCE_TOTAL, TOPK), jnp.float32) ** shard_levels(part_splits[10], (SEQUENCE_TOTAL, TOPK), ((0, 64),), -0.2, 0.2)), 0.05, 1.0)
    w_gate = normal_values(key_list[11], (EXPERTS, D, FF), D ** -0.5, 0.09375, ((0, 64), (2, 2)))
    w_up = normal_values(key_list[12], (EXPERTS, D, FF), D ** -0.5, 0.09375, ((0, 64), (2, 2)))
    w_down = normal_values(key_list[13], (EXPERTS, FF, D), (FF // 4) ** -0.5, 0.4375, ((0, 64), (1, 2)))
    return dict(queries=queries, token_keys=token_keys, token_values=token_values, stored_keys=stored_keys, stored_values=stored_values, kv_len=kv_len, residual=residual, out_weight=out_weight, norm_gain=norm_gain, expert_ids=expert_ids, route_weight=route_weight, w_gate=w_gate, w_up=w_up, w_down=w_down)


def attend(queries, token_keys, token_values, stored_keys, stored_values, kv_len):
    sequence_rows = queries.shape[0]
    query_group_width = QUERY_HEADS // KEY_VALUE_HEADS
    query_head_rows = queries.astype(jnp.float32).reshape(sequence_rows, KEY_VALUE_HEADS, query_group_width, HEAD_WIDTH)
    keys_from_cache = stored_keys.astype(jnp.float32).reshape(sequence_rows, CACHE_POSITIONS, KEY_VALUE_HEADS, HEAD_WIDTH)
    values_from_cache = stored_values.astype(jnp.float32).reshape(sequence_rows, CACHE_POSITIONS, KEY_VALUE_HEADS, HEAD_WIDTH)
    keys_latest = token_keys.astype(jnp.float32).reshape(sequence_rows, KEY_VALUE_HEADS, HEAD_WIDTH)
    values_latest = token_values.astype(jnp.float32).reshape(sequence_rows, KEY_VALUE_HEADS, HEAD_WIDTH)
    inv_root = 1.0 / math.sqrt(HEAD_WIDTH)
    cached_scores = jnp.einsum('bgqd,bpgd->bgqp', query_head_rows, keys_from_cache) * inv_root
    positions = jnp.arange(CACHE_POSITIONS, dtype=jnp.int32)
    visible = positions[None, :] < kv_len[:, None]
    cached_scores = jnp.where(visible[:, None, None, :], cached_scores, -jnp.inf)
    fresh_score = jnp.einsum('bgqd,bgd->bgq', query_head_rows, keys_latest) * inv_root
    highest = jnp.maximum(lax.optimization_barrier(jnp.max(cached_scores, axis=-1)), fresh_score)
    cached_exp = jnp.exp(cached_scores - highest[..., None])
    fresh_exp = jnp.exp(fresh_score - highest)
    totals = lax.optimization_barrier(jnp.sum(cached_exp, axis=-1)) + fresh_exp
    cached_prob = lax.optimization_barrier((cached_exp / totals[..., None]).astype(jnp.bfloat16)).astype(jnp.float32)
    fresh_prob = lax.optimization_barrier((fresh_exp / totals).astype(jnp.bfloat16)).astype(jnp.float32)
    mixed = jnp.einsum('bgqp,bpgd->bgqd', cached_prob, values_from_cache)
    mixed = mixed + fresh_prob[..., None] * values_latest[:, :, None, :]
    return mixed.reshape(sequence_rows, QUERY_HEADS * HEAD_WIDTH).astype(jnp.bfloat16)

def reference(queries, token_keys, token_values, stored_keys, stored_values, kv_len, residual, out_weight, norm_gain, expert_ids, route_weight, w_gate, w_up, w_down):
    attended = attend(queries, token_keys, token_values, stored_keys, stored_values, kv_len)
    hidden_state = residual.astype(jnp.float32) + jnp.dot(attended, out_weight, preferred_element_type=jnp.float32)
    mean_square = lax.optimization_barrier(jnp.mean(hidden_state * hidden_state, axis=-1, keepdims=True))
    normed = (hidden_state * lax.rsqrt(mean_square + 1e-06) * norm_gain.astype(jnp.float32)).astype(jnp.bfloat16)
    mixing = route_weight / lax.optimization_barrier(jnp.sum(route_weight, axis=1, keepdims=True))
    flat_ids = expert_ids.reshape(-1).astype(jnp.int32)
    row_total = flat_ids.shape[0]
    sorted_rows = jnp.argsort(flat_ids, stable=True).astype(jnp.int32)
    member = flat_ids[None, :] == jnp.arange(EXPERTS, dtype=jnp.int32)[:, None]
    counts = lax.optimization_barrier(jnp.sum(member.astype(jnp.int32), axis=1)).astype(jnp.int32)
    starts = (jnp.cumsum(counts) - counts).astype(jnp.int32)
    capacity = MOST * N_EXPERT

    def one_expert(expert):
        offsets = jnp.arange(capacity, dtype=jnp.int32)
        taken_rows = sorted_rows[jnp.clip(starts[expert] + offsets, 0, row_total - 1)]
        alive_slot = offsets < counts[expert]
        inputs = normed[taken_rows // TOPK]
        gate_act = jnp.dot(inputs, w_gate[expert], preferred_element_type=jnp.float32)
        up_act = jnp.dot(inputs, w_up[expert], preferred_element_type=jnp.float32)
        hidden_act = (jax.nn.silu(gate_act) * up_act).astype(jnp.bfloat16)
        output = jnp.dot(hidden_act, w_down[expert], preferred_element_type=jnp.float32)
        return (jnp.where(alive_slot[:, None], output, 0.0), taken_rows)
    outputs, taken_all = lax.map(one_expert, jnp.arange(EXPERTS, dtype=jnp.int32))
    weights = mixing.reshape(-1)[taken_all]
    moe_out = jnp.zeros((SEQUENCE_TOTAL, D), jnp.float32).at[(taken_all // TOPK).reshape(-1)].add((weights[..., None] * outputs).reshape(-1, D))
    return (hidden_state + moe_out).astype(jnp.bfloat16)
```

```python
import functools
import math

import jax
import jax.numpy as jnp
from jax import lax
from jax.experimental import pallas as pl
from jax.experimental.pallas import tpu as pltpu
from jax.sharding import PartitionSpec as P

HW = 128
SLOTS = 2
BF = jnp.bfloat16
F32 = jnp.float32
NEG = -jnp.inf


def dot(a, b, dims=((1,), (0,)), precision=None):
    return lax.dot_general(a, b, (dims, ((), ())), preferred_element_type=F32, precision=precision)


def iota(shape, dim):
    return lax.broadcasted_iota(jnp.int32, shape, dim)


def kernel(
    n, q_hbm, tk_hbm, tv_hbm, k_hbm, v_hbm, len_hbm, res_hbm, ow_hbm, gain_hbm, ids_hbm, rw_hbm, wg_hbm, wu_hbm, wd_hbm,
    out_ref,
    q_s, tk_s, tv_s, k_s, v_s, len_s, gain_s, ids_s, rw_s, wgu, wdo, wdp,
    wb, res, att, xs, ysend, rbuf, hid, hg, hm, hall, tsend, town, toth,
    idt, id1, idg, id2, pbuf, ctb, ss0, ss1, ss2t, ss2, sso, ssp,
    acco, accx, scr, acto, acts, actx, osend, gbuf, csend, zbuf, fsend, frecv,
    lsem, ssem, wsem, rsem, tsem1, xsem, rrsem, hmsem, hsem, tsem, osem, ss1sem, ss2sem, id1sem, id2sem, dsem, gsem, zsem,
):
    r = lax.axis_index("replica")
    e = lax.axis_index("expert")
    x, y = e // n, e % n
    u, v = x * (1 - r) + y * r, y * (1 - r) + x * r
    a, b = n - r * (n - 1), 1 + r * (n - 1)
    heads = n * n
    cols = wb.shape[3]
    half = n * cols
    lanes = 2 * HW

    def own(uu, vv):
        return {"expert": uu * a + vv * b, "replica": r}

    partner = {"expert": e, "replica": 1 - r}

    def remote(src, dst, send, recv, device):
        return pltpu.make_async_remote_copy(
            src, dst, ssem.at[send], recv, device_id=device, device_id_type=pl.DeviceIdType.MESH
        )

    def local(src, dst, sem):
        return pltpu.make_async_copy(src, dst, sem)

    def arrived(ref, sem):
        local(ref, ref, sem).wait()

    def around(w, d):
        return lax.rem(w + d, n)

    scope = jax.named_scope

    with scope("barrier"):
        bar = pltpu.get_barrier_semaphore()

        def greet(d, c):
            for rr in (0, 1):
                pl.semaphore_signal(bar, device_id={"expert": around(x, d) * n + y, "replica": rr}, device_id_type=pl.DeviceIdType.MESH)
                pl.semaphore_signal(bar, device_id={"expert": x * n + around(y, d), "replica": rr}, device_id_type=pl.DeviceIdType.MESH)
            return c

        lax.fori_loop(1, n, greet, 0)
        pl.semaphore_signal(bar, device_id=partner, device_id_type=pl.DeviceIdType.MESH)

        def qcopy(h, c):
            local(q_hbm.at[:, pl.ds(pl.multiple_of(h * HW, HW), HW)], q_s.at[h], lsem.at[0]).start()
            return c

        lax.fori_loop(0, heads, qcopy, 0)
        local(len_hbm, len_s, lsem.at[1]).start()
        local(tk_hbm, tk_s, lsem.at[2]).start()
        local(tv_hbm, tv_s, lsem.at[3]).start()
        local(ids_hbm, ids_s, lsem.at[4]).start()
        local(rw_hbm, rw_s, lsem.at[5]).start()
        local(k_hbm, k_s, lsem.at[6]).start()
        local(v_hbm, v_s, lsem.at[7]).start()
        local(gain_hbm, gain_s, lsem.at[8]).start()
        local(ow_hbm.at[:, pl.ds(pl.multiple_of(r * half + v * cols, cols), cols)], wb.at[v, r], lsem.at[9]).start()
        local(res_hbm.at[:, pl.ds(pl.multiple_of(r * half + v * cols, cols), cols)], res.at[v, r], lsem.at[10]).start()
        hidden_units = wg_hbm.shape[2]
        local(wg_hbm.at[0], wgu.at[:, pl.ds(0, hidden_units)], lsem.at[11]).start()
        local(wu_hbm.at[0], wgu.at[:, pl.ds(hidden_units, hidden_units)], lsem.at[12]).start()
        local(wd_hbm.at[0, :, pl.ds(pl.multiple_of(r * half, half), half)], wdo, lsem.at[13]).start()
        pl.semaphore_wait(bar, 4 * (n - 1) + 1)

    with scope("weights_send"):

        def wsend(d, c):
            vv = around(v, d)
            at = pl.ds(pl.multiple_of(r * half + vv * cols, cols), cols)
            remote(ow_hbm.at[:, at], wb.at[v, r], 0, wsem.at[0], own(u, vv)).start()
            return c

        def wcross(d, c):
            uu = around(u, d)
            at = pl.ds(pl.multiple_of((1 - r) * half + uu * cols, cols), cols)
            remote(ow_hbm.at[:, at], wb.at[u, r], 1, wsem.at[1], {"expert": uu * a + v * b, "replica": 1 - r}).start()
            return c

        def rsend(d, c):
            vv = around(v, d)
            at = pl.ds(pl.multiple_of(r * half + vv * cols, cols), cols)
            remote(res_hbm.at[:, at], res.at[v, r], 2, rsem.at[0], own(u, vv)).start()
            return c

        def rcross(d, c):
            uu = around(u, d)
            at = pl.ds(pl.multiple_of((1 - r) * half + uu * cols, cols), cols)
            remote(res_hbm.at[:, at], res.at[u, r], 3, rsem.at[1], {"expert": uu * a + v * b, "replica": 1 - r}).start()
            return c

        lax.fori_loop(1, n, wsend, 0)
        lax.fori_loop(0, n, wcross, 0)
        lax.fori_loop(1, n, rsend, 0)
        lax.fori_loop(0, n, rcross, 0)
        remote(wd_hbm.at[0, :, pl.ds(pl.multiple_of((1 - r) * half, half), half)], wdp, 4, dsem.at[0], partner).start()

    tok = ids_s.shape[0]
    topk = ids_s.shape[1]
    tokens = n * tok
    with scope("ids_send"):
        local(ids_hbm, ids_s, lsem.at[4]).wait()
        local(rw_hbm, rw_s, lsem.at[5]).wait()
        weight = rw_s[...]
        mixing = weight / jnp.sum(weight, axis=1, keepdims=True)
        lane = iota((tok, HW), 1)
        row = iota((tok, HW), 0)
        place = (lane == v * tok + row).astype(F32)
        place_mix = (lane == tokens + v * tok + row).astype(F32)
        exact = lax.Precision.HIGHEST
        idt[...] = dot(ids_s[...].astype(F32), place, ((0,), (0,)), exact) + dot(mixing, place_mix, ((0,), (0,)), exact)

        def id1send(d, c):
            remote(idt, id1.at[v], 5, id1sem, own(u, around(v, d))).start()
            return c

        lax.fori_loop(1, n, id1send, 0)
        id1[v] = idt[...]

    with scope("attention"):
        seqs = k_s.shape[0]
        pos = k_s.shape[1]
        kvh = k_s.shape[2] // HW
        per = heads // kvh
        rows = per * seqs
        arrived(q_s, lsem.at[0])
        local(len_hbm, len_s, lsem.at[1]).wait()
        local(tk_hbm, tk_s, lsem.at[2]).wait()
        local(tv_hbm, tv_s, lsem.at[3]).wait()
        local(k_hbm, k_s, lsem.at[6]).wait()
        inv_root = 1.0 / math.sqrt(HW)
        rowseq = lax.rem(iota((rows, pos), 0), seqs)
        colpos = iota((rows, pos), 1)
        visible = jnp.concatenate(
            [jnp.where((rowseq == s) & (colpos < len_s[s]), 0.0, NEG) for s in range(seqs)], axis=1
        )
        fresh_ok = lax.rem(iota((rows, seqs), 0), seqs) == iota((rows, seqs), 1)
        for g in range(kvh):
            at = slice(g * HW, (g + 1) * HW)
            qg = q_s[g * per : (g + 1) * per].reshape(rows, HW)
            kg = k_s[:, :, at].reshape(seqs * pos, HW)
            s_old = dot(qg, kg, ((1,), (1,))) * inv_root + visible
            s_new = jnp.where(fresh_ok, dot(qg, tk_s[:, at], ((1,), (1,))) * inv_root, NEG)
            top = jnp.maximum(jnp.max(s_old, axis=1, keepdims=True), jnp.max(s_new, axis=1, keepdims=True))
            p_old = jnp.exp(s_old - top)
            p_new = jnp.exp(s_new - top)
            scale = 1.0 / (jnp.sum(p_old, axis=1, keepdims=True) + jnp.sum(p_new, axis=1, keepdims=True))
            p_old = (p_old * scale).astype(BF)
            p_new = (p_new * scale).astype(BF).astype(F32)
            if g == 0:
                local(v_hbm, v_s, lsem.at[7]).wait()
            vg = v_s[:, :, at].reshape(seqs * pos, HW)
            mixed = dot(p_old, vg)
            tv = tv_s[:, at].astype(F32)
            for s in range(seqs):
                mixed = mixed + p_new[:, s : s + 1] * tv[s : s + 1, :]
            att[g * (n // kvh) : (g + 1) * (n // kvh)] = mixed.astype(BF).reshape(n // kvh, n, seqs, HW)

    with scope("feature_send"):

        def t1send(d, c):
            xx, yy = around(x, d), around(y, d)
            remote(att.at[xx], xs.at[y, :, pl.ds((x * 2 + r) * seqs, seqs)], 7, tsem1, {"expert": xx * n + y, "replica": 0}).start()
            remote(att.at[:, yy], xs.at[x, :, pl.ds((y * 2 + r) * seqs, seqs)], 7, tsem1, {"expert": x * n + yy, "replica": 1}).start()
            return c

        lax.fori_loop(1, n, t1send, 0)

        @pl.when(r == 0)
        def _():
            remote(att.at[:, y], xs.at[x, :, pl.ds((y * 2 + r) * seqs, seqs)], 7, tsem1, partner).start()
            local(att.at[x], xs.at[y, :, pl.ds((x * 2 + r) * seqs, seqs)], lsem.at[14]).start()

        @pl.when(r == 1)
        def _():
            remote(att.at[x], xs.at[y, :, pl.ds((x * 2 + r) * seqs, seqs)], 7, tsem1, partner).start()
            local(att.at[:, y], xs.at[x, :, pl.ds((y * 2 + r) * seqs, seqs)], lsem.at[14]).start()

    with scope("ids_second"):
        arrived(id1.at[pl.ds(0, n - 1)], id1sem)
        idg[...] = functools.reduce(lambda p, q: p + q, [id1[i] for i in range(n)])

        def id2send(d, c):
            remote(idg, id2.at[u], 6, id2sem, own(around(u, d), v)).start()
            return c

        lax.fori_loop(1, n, id2send, 0)
        id2[u] = idg[...]

    with scope("feature_gather"):
        arrived(att.at[0], lsem.at[14])
        arrived(xs.at[0, :, pl.ds(0, (2 * n - 1) * seqs)], tsem1)

        def t2send(d, c):
            remote(xs.at[v], xs.at[v], 8, xsem.at[v], own(u, around(v, d))).start()
            return c

        lax.fori_loop(1, n, t2send, 0)

    with scope("tables"):
        arrived(id2.at[pl.ds(0, n - 1)], id2sem)
        block = (iota((n, HW), 1) // tok == iota((n, HW), 0)).astype(F32)
        before = (
            (iota((HW, HW), 0) // tok == iota((HW, HW), 1) // tok) & (iota((HW, HW), 0) < iota((HW, HW), 1))
        ).astype(BF)
        place_v = iota((n, 1), 0).astype(F32)
        ue = u.astype(F32)
        ve = v.astype(F32)
        ae = a.astype(F32)
        be = b.astype(F32)
        expert_v = ae * ue + be * place_v
        named = []
        for i in range(n):
            got = id2[i]
            named.append(functools.reduce(lambda p, q: p + q, [(got[k : k + 1] == expert_v).astype(F32) for k in range(topk)]))
        named = jnp.concatenate(named, axis=0)
        rank = dot(named.astype(BF), before)
        for i in range(n):
            here = slice(i * n, (i + 1) * n)
            picks = []
            for j in range(SLOTS):
                hit = jnp.where(rank[here] == j, named[here], 0.0)
                picks.append(hit[:, None, :] * block[None])
            pbuf[i] = jnp.stack(picks, axis=1).reshape(HW, HW).astype(BF)
        got = idg[...]
        back = pltpu.roll(got, tokens, 1)
        expert_u = ae * place_v + be * ve
        same = [got[k : k + 1] == expert_u for k in range(topk)]
        chosen = functools.reduce(lambda p, q: p + q, [s.astype(F32) for s in same])
        mix = functools.reduce(lambda p, q: p + q, [jnp.where(s, back[k : k + 1], 0.0) for k, s in enumerate(same)])
        rank = dot(jnp.concatenate([chosen, chosen], axis=0).astype(BF), before)[:n]
        picks = []
        for j in range(SLOTS):
            hit = jnp.where(rank == j, mix, 0.0)
            picks.append(hit[:, None, :] * block[None])
        table = jnp.stack(picks, axis=1).reshape(HW, HW)
        high = table.astype(BF)
        low = (table - high.astype(F32)).astype(BF)
        ctb[...] = jnp.concatenate([high[:, :tokens], low[:, :tokens]], axis=1)

    with scope("project"):
        local(ow_hbm.at[:, pl.ds(0, cols)], wb.at[v, r], lsem.at[9]).wait()
        arrived(wb.at[pl.ds(0, n - 1), 0], wsem.at[0])
        arrived(wb.at[:, 0], wsem.at[1])
        wv = wb.reshape(n * HW, cols)

        def project(i, c):
            odd = lax.rem(i, 2)
            d = odd * ((i + 1) // 2) + (1 - odd) * (n - i // 2)
            vv = around(v, d)

            @pl.when(i > 0)
            def _():
                arrived(xs.at[vv], xsem.at[vv])

            lhs = jnp.concatenate([xs[vv, k] for k in range(n)], axis=1)
            part = dot(lhs, wv[...])
            ysend[:, vv] = part.astype(BF).reshape(n, tok, cols)
            return c

        lax.fori_loop(0, n, project, 0)

    with scope("reduce_send"):

        def ysend_to(d, c):
            uu = around(u, d)
            remote(ysend.at[uu], rbuf.at[u], 9, rrsem, own(uu, v)).start()
            return c

        lax.fori_loop(1, n, ysend_to, 0)
        rbuf[u] = ysend[u]
        local(res_hbm.at[:, pl.ds(0, cols)], res.at[v, r], lsem.at[10]).wait()
        arrived(res.at[pl.ds(0, n - 1), 0], rsem.at[0])
        arrived(res.at[:, 0], rsem.at[1])
        local(gain_hbm, gain_s, lsem.at[8]).wait()
    with scope("reduce_wait"):
        arrived(rbuf.at[pl.ds(0, n - 1)], rrsem)
    with scope("hidden"):
        total = res[...].astype(F32).reshape(n * tok, cols)
        for i in range(n):
            total = total + rbuf[i].astype(F32).reshape(tokens, cols)
        hid[...] = total.reshape(n, tok, cols)
        gain = gain_s[pl.ds(pl.multiple_of(r * half + v * cols, cols), cols)].astype(F32).reshape(1, cols)
        hg[...] = (total * gain).astype(BF)

        def d1send(d, c):
            remote(hg, hall.at[u], 10, hsem.at[u], own(around(u, d), v)).start()
            return c

        lax.fori_loop(1, n, d1send, 0)
        hall[u] = hg[...]
        square = (total * total).astype(BF)
        sums = dot(jnp.ones((n, cols), BF), square, ((1,), (1,)))
        ss0[...] = jnp.concatenate([sums, jnp.zeros((n, HW - tokens), F32)], axis=1)

        def ss1send(d, c):
            vv = around(v, d)
            remote(ss0, ss1.at[v], 11, ss1sem, own(u, vv)).start()
            remote(hid.at[vv], hm.at[v], 12, hmsem, own(u, vv)).start()
            return c

        lax.fori_loop(1, n, ss1send, 0)
        ss1[v] = ss0[...]
        hm[v] = hid[v]

    with scope("dispatch"):

        def pack(i, c):
            odd = lax.rem(i, 2)
            d = odd * ((i + 1) // 2) + (1 - odd) * (n - i // 2)
            uu = around(u, d)

            @pl.when(i > 0)
            def _():
                arrived(hall.at[uu], hsem.at[uu])

            slots = dot(pbuf[uu, :, pl.ds(0, tokens)], hall[uu]).astype(BF)
            tsend[uu] = slots.reshape(n, SLOTS * n, cols)

            def to(dd, cc):
                vv = around(v, dd)
                remote(tsend.at[uu, vv], town.at[v, uu], 13, tsem.at[v], own(u, vv)).start()
                return cc

            lax.fori_loop(1, n, to, 0)
            town[v, uu] = tsend[uu, v]
            return c

        lax.fori_loop(0, n, pack, 0)

    with scope("sums_second"):
        arrived(ss1.at[pl.ds(0, n - 1)], ss1sem)
        ss2t[...] = functools.reduce(lambda p, q: p + q, [ss1[i] for i in range(n)])

        def ss2send(d, c):
            remote(ss2t, ss2.at[u], 14, ss2sem, own(around(u, d), v)).start()
            return c

        lax.fori_loop(1, n, ss2send, 0)
        ss2[u] = ss2t[...]

    with scope("weights_wait"):
        local(wg_hbm.at[0], wgu.at[:, pl.ds(0, hidden_units)], lsem.at[11]).wait()
        local(wu_hbm.at[0], wgu.at[:, pl.ds(0, hidden_units)], lsem.at[12]).wait()
        acco[...] = jnp.zeros_like(acco)
        accx[...] = jnp.zeros_like(accx)
        tiles = accx.shape[0]
        tv_own = town.reshape(n, HW, cols)
        tv_oth = toth.reshape(n, HW, cols)
    with scope("gate_up_own"):

        def gate_own(i, c):
            odd = lax.rem(i, 2)
            d = odd * ((i + 1) // 2) + (1 - odd) * (n - i // 2)
            vv = around(v, d)

            @pl.when(i > 0)
            def _():
                arrived(town.at[vv], tsem.at[vv])

            remote(town.at[vv], toth.at[i], 15, osem.at[i], partner).start()
            at = pl.ds(pl.multiple_of(r * half + vv * cols, cols), cols)
            acco[...] += dot(tv_own[vv], wgu[at, :])
            return c

        lax.fori_loop(0, n, gate_own, 0)
    with scope("gate_up_other"):

        def gate_other(i, c):
            odd = lax.rem(i, 2)
            d = odd * ((i + 1) // 2) + (1 - odd) * (n - i // 2)
            uu = around(u, d)
            arrived(toth.at[i], osem.at[i])
            at = pl.ds(pl.multiple_of((1 - r) * half + uu * cols, cols), cols)
            part = dot(tv_oth[i], wgu[at, :])
            for t in range(tiles):
                accx[t] += part[:, t * HW : (t + 1) * HW]
            return c

        lax.fori_loop(0, n, gate_other, 0)

    with scope("sums_third"):
        arrived(ss2.at[pl.ds(0, n - 1)], ss2sem)
        for i in range(n):
            mine = pbuf[i, pl.ds(pl.multiple_of(v * SLOTS * n, SLOTS * n), SLOTS * n), :].astype(F32)
            column = jnp.sum(mine * ss2[i][0:1], axis=1, keepdims=True)
            sso[i * SLOTS * n : (i + 1) * SLOTS * n, :] = jnp.broadcast_to(column, (SLOTS * n, HW))
        remote(sso, ssp, 16, dsem.at[1], partner).start()
        arrived(ssp, dsem.at[1])

    with scope("activation"):

        def swapped(ref):
            return jnp.concatenate(
                [ref[pl.ds(j * n + i, n, stride=SLOTS * n), :] for i in range(n) for j in range(SLOTS)], axis=0
            )

        model = 2 * half
        scale = lax.rsqrt((sso[...] + swapped(ssp)) * (1.0 / model) + 1e-06)
        up_at = tiles // 2
        for t in range(up_at):
            gate = (acco[:, t * HW : (t + 1) * HW] + swapped(accx.at[t])) * scale
            up = (acco[:, (t + up_at) * HW : (t + up_at + 1) * HW] + swapped(accx.at[t + up_at])) * scale
            act = gate / (1.0 + jnp.exp(-gate)) * up
            acto[:, t * HW : (t + 1) * HW] = act.astype(BF)
            scr[t] = act
        for t in range(up_at):
            acts[:, t * HW : (t + 1) * HW] = swapped(scr.at[t]).astype(BF)
        remote(acts, actx, 17, dsem.at[2], partner).start()
        local(wd_hbm.at[0, :, pl.ds(0, half)], wdo, lsem.at[13]).wait()
        arrived(wdp, dsem.at[0])
        arrived(actx, dsem.at[2])

    with scope("down"):
        osv = osend.reshape(HW, half)

        def down(i, c):
            at = pl.ds(pl.multiple_of(i * cols, cols), cols)
            osv[:, at] = (dot(acto[...], wdo[:, at]) + dot(actx[...], wdp[:, at])).astype(BF)
            return c

        lax.fori_loop(0, n, down, 0)

        def gsend(d, c):
            uu = around(u, d)
            remote(osend.at[uu], gbuf.at[u], 18, gsem, own(uu, v)).start()
            return c

        lax.fori_loop(1, n, gsend, 0)
        gbuf[u] = osend[u]
    with scope("return_wait"):
        arrived(gbuf.at[pl.ds(0, n - 1)], gsem)
    with scope("combine"):
        gv = gbuf.reshape(HW, half)

        def combine(i, c):
            at = pl.ds(pl.multiple_of(i * cols, cols), cols)
            both = dot(ctb[...], gv[:, at], ((0,), (0,)))
            csend[:, :, at] = (both[:tokens] + both[tokens:]).astype(BF).reshape(n, tok, cols)
            return c

        lax.fori_loop(0, n, combine, 0)

        def zsend(d, c):
            vv = around(v, d)
            remote(csend.at[vv], zbuf.at[v], 19, zsem, own(u, vv)).start()
            return c

        lax.fori_loop(1, n, zsend, 0)
        zbuf[v] = csend[v]
        arrived(hm.at[pl.ds(0, n - 1)], hmsem)
    with scope("home_wait"):
        arrived(zbuf.at[pl.ds(0, n - 1)], zsem)
    with scope("final"):
        mine = tok // 2
        for i in range(n):
            at = slice(i * cols, (i + 1) * cols)
            total = hm[i]
            for j in range(n):
                total = total + zbuf[j, :, at].astype(F32)
            keep = jnp.where(r == 0, total[:mine], total[mine:])
            give = jnp.where(r == 0, total[mine:], total[:mine])
            out_ref[:, pl.ds(pl.multiple_of(r * half + i * cols, cols), cols)] = keep.astype(BF)
            fsend[:, at] = give.astype(BF)
        remote(fsend, frecv, 20, dsem.at[3], partner).start()
        arrived(frecv, dsem.at[3])
        out_ref[:, pl.ds(pl.multiple_of((1 - r) * half, half), half)] = frecv[...]

    with scope("drain"):

        most = pl.ds(0, n - 1)
        for send, ref in enumerate((
            wb.at[most, 0], wb.at[:, 0], res.at[most, 0], res.at[:, 0], wdp, id1.at[most], id2.at[most],
            xs.at[0, :, pl.ds(0, (2 * n - 1) * seqs)], xs.at[most], rbuf.at[most], hall.at[most], ss1.at[most], hm.at[most],
            town.at[most], ss2.at[most], town, sso, acts, gbuf.at[most], zbuf.at[most], fsend,
        )):
            arrived(ref, ssem.at[send])


def solution(mesh):
    n = math.isqrt(mesh.shape["expert"])

    def on_device(queries, token_keys, token_values, stored_keys, stored_values, kv_len, residual, out_weight, norm_gain,
                  expert_ids, route_weight, w_gate, w_up, w_down):
        seqs, pos, kvw = stored_keys.shape
        heads = queries.shape[1] // HW
        model = residual.shape[1]
        half = model // 2
        cols = half // n
        tok, topk = expert_ids.shape
        hidden = w_gate.shape[2]
        tokens = n * tok
        slots = SLOTS * n
        tiles = 2 * hidden // HW
        wrows = out_weight.shape[0]
        vmem = pltpu.VMEM
        dma = pltpu.SemaphoreType.DMA
        scratch = [
            vmem((heads, seqs, HW), BF), vmem((seqs, kvw), BF), vmem((seqs, kvw), BF),
            vmem((seqs, pos, kvw), BF), vmem((seqs, pos, kvw), BF), pltpu.SMEM((seqs,), jnp.int32),
            vmem((model,), BF), vmem((tok, topk), jnp.int32), vmem((tok, topk), F32),
            vmem((model, 2 * hidden), BF), vmem((hidden, half), BF), vmem((hidden, half), BF),
            vmem((n, 2, wrows, cols), BF), vmem((n, 2, seqs, cols), BF),
            vmem((n, n, seqs, HW), BF), vmem((n, n, tokens, HW), BF),
            vmem((n, n, tok, cols), BF), vmem((n, n, tok, cols), BF),
            vmem((n, tok, cols), F32), vmem((tokens, cols), BF), vmem((n, tok, cols), F32),
            vmem((n, tokens, cols), BF), vmem((n, n, slots, cols), BF), vmem((n, n, slots, cols), BF), vmem((n, n, slots, cols), BF),
            vmem((topk, HW), F32), vmem((n, topk, HW), F32), vmem((topk, HW), F32), vmem((n, topk, HW), F32),
            vmem((n, HW, HW), BF), vmem((HW, 2 * tokens), BF),
            vmem((n, HW), F32), vmem((n, n, HW), F32), vmem((n, HW), F32), vmem((n, n, HW), F32),
            vmem((HW, HW), F32), vmem((HW, HW), F32),
            vmem((HW, 2 * hidden), F32), vmem((tiles, HW, HW), F32), vmem((tiles // 2, HW, HW), F32),
            vmem((HW, hidden), BF), vmem((HW, hidden), BF), vmem((HW, hidden), BF),
            vmem((n, slots, half), BF), vmem((n, slots, half), BF),
            vmem((n, tok, half), BF), vmem((n, tok, half), BF), vmem((tok // 2, half), BF), vmem((tok // 2, half), BF),
            dma((15,)), dma((21,)), dma((2,)), dma((2,)), dma, dma((n,)), dma, dma, dma((n,)), dma((n,)), dma((n,)), dma, dma, dma, dma, dma((4,)), dma, dma,
        ]
        return pl.pallas_call(
            functools.partial(kernel, n),
            out_shape=jax.ShapeDtypeStruct(residual.shape, BF),
            in_specs=[pl.BlockSpec(memory_space=pl.ANY)] * 14,
            out_specs=pl.BlockSpec(memory_space=pltpu.VMEM),
            scratch_shapes=scratch,
            compiler_params=pltpu.CompilerParams(
                collective_id=0, has_side_effects=True, vmem_limit_bytes=60 * 1024 * 1024
            ),
        )(queries, token_keys, token_values, stored_keys, stored_values, kv_len, residual, out_weight, norm_gain,
          expert_ids, route_weight, w_gate, w_up, w_down)

    everyone = ("groups", "expert", "replica")
    in_specs = (
        P(everyone, None), P(everyone, None), P(everyone, None), P(everyone, None, None), P(everyone, None, None),
        P(everyone), P(everyone, None), P(("expert", "replica"), None), P(), P(("groups", "expert"), None),
        P(("groups", "expert"), None), P("expert", None, "replica"), P("expert", None, "replica"), P("expert", "replica", None),
    )
    return jax.shard_map(
        on_device, mesh=mesh, in_specs=in_specs, out_specs=P(everyone, None), check_vma=False
    )
```

```python
import functools
import math

import jax
import jax.numpy as jnp
from jax import lax
from jax.experimental import pallas as pl
from jax.experimental.pallas import tpu as pltpu
from jax.sharding import PartitionSpec as P

HW = 128
SLOTS = 2
BF = jnp.bfloat16
F32 = jnp.float32
NEG = -jnp.inf


def dot(a, b, dims=((1,), (0,)), precision=None):
    return lax.dot_general(a, b, (dims, ((), ())), preferred_element_type=F32, precision=precision)


def iota(shape, dim):
    return lax.broadcasted_iota(jnp.int32, shape, dim)


def kernel(
    n, q_hbm, tk_hbm, tv_hbm, k_hbm, v_hbm, len_hbm, res_hbm, ow_hbm, gain_hbm, ids_hbm, rw_hbm, wg_hbm, wu_hbm, wd_hbm,
    out_ref,
    q_s, tk_s, tv_s, k_s, v_s, len_s, gain_s, ids_s, rw_s, wgu, wdn,
    wb, res, att, xs, ysend, rbuf, hid, hg, hm, hall, tsend, town, toth,
    idt, id1, idg, id2, pbuf, ctb, ss0, ss1, ss2t, ss2, sso, ssp,
    acco, accx, scr, acto, acts, actx, osend, gbuf, csend, zbuf,
    lsem, ssem, wsem, rsem, t1sem, xsem, rrsem, hmsem, hsem, tsem, osem, ss1sem, ss2sem, id1sem, id2sem, dsem, gsem, zsem,
):
    r = lax.axis_index("replica")
    e = lax.axis_index("expert")
    x, y = e // n, e % n
    u, v = x * (1 - r) + y * r, y * (1 - r) + x * r
    a, b = n - r * (n - 1), 1 + r * (n - 1)
    heads = n * n
    cols = wb.shape[3]
    half = n * cols
    seqs, pos = k_s.shape[0], k_s.shape[1]
    tok, topk = ids_s.shape
    tokens = n * tok
    slots = SLOTS * n
    most = pl.ds(0, n - 1)
    mesh_id = pl.DeviceIdType.MESH

    def own(uu, vv):
        return {"expert": uu * a + vv * b, "replica": r}

    def across(uu, vv):
        return {"expert": uu * a + vv * b, "replica": 1 - r}

    partner = {"expert": e, "replica": 1 - r}

    def remote(src, dst, send, recv, device):
        return pltpu.make_async_remote_copy(src, dst, ssem.at[send], recv, device_id=device, device_id_type=mesh_id)

    def local(src, dst, sem):
        return pltpu.make_async_copy(src, dst, sem)

    def arrived(ref, sem):
        local(ref, ref, sem).wait()

    def around(w, d):
        return lax.rem(w + d, n)

    def far(i):
        return n // 2 + (2 * lax.rem(i, 2) - 1) * (i // 2)

    def each(body):
        def step(i, c):
            body(far(i), c)
            return c

        lax.fori_loop(1, n, step, 0)

    def columns(plane, block):
        return pl.ds(pl.multiple_of(plane * half + block * cols, cols), cols)

    scope = jax.named_scope

    with scope("barrier"):
        bar = pltpu.get_barrier_semaphore()

        def greet(d, c):
            for rr in (0, 1):
                pl.semaphore_signal(bar, device_id={"expert": around(x, d) * n + y, "replica": rr}, device_id_type=mesh_id)
                pl.semaphore_signal(bar, device_id={"expert": x * n + around(y, d), "replica": rr}, device_id_type=mesh_id)
            return c

        lax.fori_loop(1, n, greet, 0)
        pl.semaphore_signal(bar, device_id=partner, device_id_type=mesh_id)

        def qcopy(h, c):
            local(q_hbm.at[:, pl.ds(pl.multiple_of(h * HW, HW), HW)], q_s.at[h], lsem.at[0]).start()
            return c

        lax.fori_loop(0, heads, qcopy, 0)
        local(ids_hbm, ids_s, lsem.at[4]).start()
        local(rw_hbm, rw_s, lsem.at[5]).start()
        local(len_hbm, len_s, lsem.at[1]).start()
        local(tk_hbm, tk_s, lsem.at[2]).start()
        local(tv_hbm, tv_s, lsem.at[3]).start()
        local(k_hbm, k_s, lsem.at[6]).start()
        local(v_hbm, v_s, lsem.at[7]).start()
        local(ow_hbm.at[:, columns(r, v)], wb.at[v, r], lsem.at[9]).start()
        local(res_hbm.at[:, columns(r, v)], res.at[v, r], lsem.at[10]).start()
        local(gain_hbm, gain_s, lsem.at[8]).start()
        units = wg_hbm.shape[2]
        first_units, last_units = pl.ds(0, units), pl.ds(units, units)
        local(wg_hbm.at[0], wgu.at[:, first_units], lsem.at[11]).start()
        local(wu_hbm.at[0], wgu.at[:, last_units], lsem.at[12]).start()
        local(wd_hbm.at[0, :, pl.ds(pl.multiple_of(r * half, half), half)], wdn.at[first_units], lsem.at[13]).start()

    with scope("ids"):
        local(ids_hbm, ids_s, lsem.at[4]).wait()
        local(rw_hbm, rw_s, lsem.at[5]).wait()
        weight = rw_s[...]
        mixing = weight / jnp.sum(weight, axis=1, keepdims=True)
        lane = iota((tok, HW), 1)
        row = iota((tok, HW), 0)
        place = (lane == v * tok + row).astype(F32)
        place_mix = (lane == tokens + v * tok + row).astype(F32)
        exact = lax.Precision.HIGHEST
        idt[...] = dot(ids_s[...].astype(F32), place, ((0,), (0,)), exact) + dot(mixing, place_mix, ((0,), (0,)), exact)
        id1[v] = idt[...]
    with scope("barrier_wait"):
        pl.semaphore_wait(bar, 4 * (n - 1) + 1)

    with scope("weights_send"):

        def wsend(d, c):
            vv, uu = around(v, d), around(u, d)
            remote(idt, id1.at[v], 5, id1sem, own(u, vv)).start()
            remote(ow_hbm.at[:, columns(r, vv)], wb.at[v, r], 0, wsem.at[0], own(u, vv)).start()
            remote(ow_hbm.at[:, columns(1 - r, uu)], wb.at[u, r], 1, wsem.at[1], across(uu, v)).start()

        each(wsend)
        remote(ow_hbm.at[:, columns(1 - r, u)], wb.at[u, r], 1, wsem.at[1], partner).start()

    with scope("attention"):
        kvh = k_s.shape[2] // HW
        per = heads // kvh
        rows = per * seqs
        arrived(q_s, lsem.at[0])
        local(len_hbm, len_s, lsem.at[1]).wait()
        local(tk_hbm, tk_s, lsem.at[2]).wait()
        local(tv_hbm, tv_s, lsem.at[3]).wait()
        local(k_hbm, k_s, lsem.at[6]).wait()
        inv_root = 1.0 / math.sqrt(HW)
        rowseq = lax.rem(iota((rows, pos), 0), seqs)
        colpos = iota((rows, pos), 1)
        visible = jnp.concatenate(
            [jnp.where((rowseq == s) & (colpos < len_s[s]), 0.0, NEG) for s in range(seqs)], axis=1
        )
        fresh_ok = lax.rem(iota((rows, seqs), 0), seqs) == iota((rows, seqs), 1)
        for g in range(kvh):
            at = slice(g * HW, (g + 1) * HW)
            qg = q_s[g * per : (g + 1) * per].reshape(rows, HW)
            kg = k_s[:, :, at].reshape(seqs * pos, HW)
            s_old = dot(qg, kg, ((1,), (1,))) * inv_root + visible
            s_new = jnp.where(fresh_ok, dot(qg, tk_s[:, at], ((1,), (1,))) * inv_root, NEG)
            top = jnp.maximum(jnp.max(s_old, axis=1, keepdims=True), jnp.max(s_new, axis=1, keepdims=True))
            p_old = jnp.exp(s_old - top)
            p_new = jnp.exp(s_new - top)
            scale = 1.0 / (jnp.sum(p_old, axis=1, keepdims=True) + jnp.sum(p_new, axis=1, keepdims=True))
            p_old = (p_old * scale).astype(BF)
            p_new = (p_new * scale).astype(BF).astype(F32)
            if g == 0:
                local(v_hbm, v_s, lsem.at[7]).wait()
            vg = v_s[:, :, at].reshape(seqs * pos, HW)
            mixed = dot(p_old, vg)
            tv = tv_s[:, at].astype(F32)
            for s in range(seqs):
                mixed = mixed + p_new[:, s : s + 1] * tv[s : s + 1, :]
            att[g * (n // kvh) : (g + 1) * (n // kvh)] = mixed.astype(BF).reshape(n // kvh, n, seqs, HW)

    with scope("feature_send"):
        mine = pl.ds(r * seqs, seqs)

        def t1send(d, c):
            xx, yy = around(x, d), around(y, d)
            ahead = d // (n // 2)
            place = ahead * (2 * (n - d) - 1) + (1 - ahead) * 2 * d
            rows_at = pl.ds(place * tok + r * seqs, seqs)
            remote(att.at[xx], xs.at[y, :, rows_at], 7, t1sem.at[place], {"expert": xx * n + y, "replica": 0}).start()
            remote(att.at[:, yy], xs.at[x, :, rows_at], 7, t1sem.at[place], {"expert": x * n + yy, "replica": 1}).start()

        each(t1send)

        @pl.when(r == 0)
        def _():
            remote(att.at[:, y], xs.at[x, :, mine], 7, t1sem.at[0], partner).start()
            local(att.at[x], xs.at[y, :, mine], lsem.at[14]).start()

        @pl.when(r == 1)
        def _():
            remote(att.at[x], xs.at[y, :, mine], 7, t1sem.at[0], partner).start()
            local(att.at[:, y], xs.at[x, :, mine], lsem.at[14]).start()

        arrived(att.at[0], lsem.at[14])

        def rsend(d, c):
            vv, uu = around(v, d), around(u, d)
            remote(res_hbm.at[:, columns(r, vv)], res.at[v, r], 2, rsem.at[0], own(u, vv)).start()
            remote(res_hbm.at[:, columns(1 - r, uu)], res.at[u, r], 3, rsem.at[1], across(uu, v)).start()

        each(rsend)
        remote(res_hbm.at[:, columns(1 - r, u)], res.at[u, r], 3, rsem.at[1], partner).start()
        remote(wd_hbm.at[0, :, pl.ds(pl.multiple_of((1 - r) * half, half), half)], wdn.at[last_units], 4, dsem.at[0], partner).start()

    chunks = n // 2
    crows = tokens // chunks

    def chunk_of(w, c):
        return xs.at[w, :, pl.ds(c * crows, crows)]

    def pass_on(w, c, d):
        remote(chunk_of(w, c), chunk_of(w, c), 8, xsem.at[w, c], own(u, around(v, d))).start()

    def start_chunk(c):
        for place in (2 * c, 2 * c + 1):
            if place == 0:
                arrived(att.at[0], t1sem.at[0])
            else:
                arrived(att.at[pl.ds(0, 2)], t1sem.at[place])
        pass_on(v, c, 1)
        pass_on(v, c, n - 1)

    def relay(s, c):
        behind, ahead = around(v, n - s), around(v, s)
        arrived(chunk_of(behind, c), xsem.at[behind, c])
        if s < n // 2 - 1 or c % 2 == 0:
            pass_on(behind, c, 1)
        arrived(chunk_of(ahead, c), xsem.at[ahead, c])
        if s < n // 2 - 1 or c % 2 == 1:
            pass_on(ahead, c, n - 1)

    wv = wb.reshape(n * HW, cols)

    def project(blocks):
        lhs = jnp.concatenate(
            [jnp.concatenate([xs[w, k] for k in range(n)], axis=1) for w in blocks], axis=0
        )
        part = dot(lhs, wv[...]).astype(BF)
        for i, w in enumerate(blocks):
            ysend[:, w] = part[i * tokens : (i + 1) * tokens].reshape(n, tok, cols)
            rbuf[u, w] = ysend[0, w]

        def to(d, c):
            uu = around(u, d)
            ahead = d // (n // 2 + 1)
            place = (1 - ahead) * (2 * d - 1) + ahead * 2 * (n - d)
            for w in blocks:
                remote(ysend.at[place, w], rbuf.at[u, w], 9, rrsem, own(uu, v)).start()

        each(to)

    with scope("gather_start"):
        start_chunk(0)
        start_chunk(1)
        start_chunk(2)
        relay(1, 0)
        start_chunk(3)
        relay(1, 1)
        relay(1, 2)
        relay(1, 3)
    with scope("weights_wait"):
        local(ow_hbm.at[:, columns(r, v)], wb.at[v, r], lsem.at[9]).wait()
        arrived(wb.at[most, 0], wsem.at[0])
        arrived(wb.at[:, 0], wsem.at[1])
    with scope("project0"):
        project([v])
    with scope("relay2"):
        for c in range(chunks):
            relay(2, c)
    with scope("project1"):
        project([around(v, 1), around(v, n - 1)])
    with scope("relay3"):
        for c in range(chunks):
            relay(3, c)
    with scope("project2"):
        project([around(v, 2), around(v, n - 2)])
    with scope("ids_second"):
        arrived(id1.at[most], id1sem)
        idg[...] = functools.reduce(lambda p, q: p + q, [id1[i] for i in range(n)])

        def id2send(d, c):
            remote(idg, id2.at[u], 6, id2sem, own(around(u, d), v)).start()

        each(id2send)
        id2[u] = idg[...]
    with scope("project3"):
        project([around(v, 3), around(v, n - 3)])
    with scope("relay4"):
        opposite = around(v, n // 2)
        for c in range(chunks):
            arrived(chunk_of(opposite, c), xsem.at[opposite, c])
    with scope("project4"):
        project([opposite])

    with scope("tables_wait"):
        arrived(id2.at[most], id2sem)
    with scope("tables"):
        block = (iota((n, HW), 1) // tok == iota((n, HW), 0)).astype(F32)
        before = (
            (iota((HW, HW), 0) // tok == iota((HW, HW), 1) // tok) & (iota((HW, HW), 0) < iota((HW, HW), 1))
        ).astype(BF)
        place_v = iota((n, 1), 0).astype(F32)
        ue = u.astype(F32)
        ve = v.astype(F32)
        ae = a.astype(F32)
        be = b.astype(F32)
        expert_v = ae * ue + be * place_v
        named = []
        for i in range(n):
            got = id2[i]
            named.append(functools.reduce(lambda p, q: p + q, [(got[k : k + 1] == expert_v).astype(F32) for k in range(topk)]))
        named = jnp.concatenate(named, axis=0)
        rank = dot(named.astype(BF), before)
        for i in range(n):
            here = slice(i * n, (i + 1) * n)
            picks = []
            for j in range(SLOTS):
                hit = jnp.where(rank[here] == j, named[here], 0.0)
                picks.append(hit[:, None, :] * block[None])
            pbuf[i] = jnp.stack(picks, axis=1).reshape(HW, HW).astype(BF)
        got = idg[...]
        back = pltpu.roll(got, tokens, 1)
        expert_u = ae * place_v + be * ve
        same = [got[k : k + 1] == expert_u for k in range(topk)]
        chosen = functools.reduce(lambda p, q: p + q, [s.astype(F32) for s in same])
        mix = functools.reduce(lambda p, q: p + q, [jnp.where(s, back[k : k + 1], 0.0) for k, s in enumerate(same)])
        rank = dot(jnp.concatenate([chosen, chosen], axis=0).astype(BF), before)[:n]
        picks = []
        for j in range(SLOTS):
            hit = jnp.where(rank == j, mix, 0.0)
            picks.append(hit[:, None, :] * block[None])
        table = jnp.stack(picks, axis=1).reshape(HW, HW)
        high = table.astype(BF)
        low = (table - high.astype(F32)).astype(BF)
        ctb[...] = jnp.concatenate([high[:, :tokens], low[:, :tokens]], axis=1)

    with scope("residual_wait"):
        local(res_hbm.at[:, columns(r, v)], res.at[v, r], lsem.at[10]).wait()
        arrived(res.at[most, 0], rsem.at[0])
        arrived(res.at[:, 0], rsem.at[1])
        local(gain_hbm, gain_s, lsem.at[8]).wait()
        gain = gain_s[columns(r, v)].astype(F32).reshape(1, cols)
    with scope("reduce_wait"):
        arrived(rbuf.at[most], rrsem)
    with scope("hidden"):
        total = res[...].astype(F32).reshape(tokens, cols)
        for i in range(n):
            total = total + rbuf[i].astype(F32).reshape(tokens, cols)
        hg[...] = (total * gain).astype(BF)
        hall[u] = hg[...]

        def d1send(i, c):
            d = far(n - i)
            uu = around(u, d)
            remote(hg, hall.at[u], 10, hsem.at[u], own(uu, v)).start()
            return c

        lax.fori_loop(1, n, d1send, 0)
        hid[...] = total.reshape(n, tok, cols)
        square = (total * total).astype(BF)
        sums = dot(jnp.ones((n, cols), BF), square, ((1,), (1,)))
        ss0[...] = jnp.concatenate([sums, jnp.zeros((n, HW - tokens), F32)], axis=1)
        ss1[v] = ss0[...]

        def ss1send(d, c):
            remote(ss0, ss1.at[v], 11, ss1sem, own(u, around(v, d))).start()

        each(ss1send)

    def pack(groups):
        for uu in groups:
            tsend[uu] = dot(pbuf[uu, :, pl.ds(0, tokens)], hall[uu]).astype(BF).reshape(n, slots, cols)

        def to(d, c):
            vv = around(v, d)
            for uu in groups:
                remote(tsend.at[uu, vv], town.at[v, uu], 13, tsem.at[uu], own(u, vv)).start()

        each(to)
        for uu in groups:
            town[v, uu] = tsend[uu, v]

    def pair(s):
        if s == 0:
            return [u]
        if 2 * s == n:
            return [around(u, s)]
        return [around(u, s), around(u, n - s)]

    def pack_pair(s):
        for uu in pair(s):
            if s > 0:
                arrived(hall.at[uu], hsem.at[uu])
        pack(pair(s))

    def hand_over(s):
        for uu in pair(s):
            arrived(town.at[most, uu], tsem.at[uu])
            remote(town.at[:, uu], toth.at[:, uu], 15, osem.at[uu], partner).start()

    with scope("pack0"):
        pack_pair(0)
    with scope("pack1"):
        pack_pair(1)

        def hmsend(d, c):
            vv = around(v, d)
            remote(hid.at[vv, mine], hm.at[0, v], 12, hmsem.at[0], own(u, vv)).start()
            remote(hid.at[vv, pl.ds((1 - r) * seqs, seqs)], hm.at[1, v], 16, hmsem.at[1], across(u, vv)).start()

        each(hmsend)
        remote(hid.at[v, pl.ds((1 - r) * seqs, seqs)], hm.at[1, v], 16, hmsem.at[1], partner).start()
        local(hid.at[v, mine], hm.at[0, v], lsem.at[1]).start()
        arrived(hm.at[0, 0], lsem.at[1])
    with scope("pack2"):
        pack_pair(2)
    with scope("pack3"):
        pack_pair(3)
    with scope("sums_second"):
        arrived(ss1.at[most], ss1sem)
        ss2t[...] = functools.reduce(lambda p, q: p + q, [ss1[i] for i in range(n)])

        def ss2send(d, c):
            remote(ss2t, ss2.at[u], 14, ss2sem, own(around(u, d), v)).start()

        each(ss2send)
        ss2[u] = ss2t[...]
    with scope("pack4"):
        pack_pair(4)
    with scope("hand0"):
        hand_over(0)
        hand_over(1)
        hand_over(2)
    with scope("expert_weights"):
        local(wg_hbm.at[0], wgu.at[:, first_units], lsem.at[11]).wait()
        local(wu_hbm.at[0], wgu.at[:, last_units], lsem.at[12]).wait()
    with scope("hand3"):
        hand_over(3)
    with scope("hand4"):
        hand_over(4)
    with scope("sums_third"):
        arrived(ss2.at[most], ss2sem)
        for i in range(n):
            part = pbuf[i, pl.ds(pl.multiple_of(v * slots, slots), slots), :].astype(F32)
            column = jnp.sum(part * ss2[i][0:1], axis=1, keepdims=True)
            sso[i * slots : (i + 1) * slots, :] = jnp.broadcast_to(column, (slots, HW))
        remote(sso, ssp, 17, dsem.at[1], partner).start()
    with scope("gate_up_own"):
        tiles = accx.shape[0]
        tv_own = town.reshape(n, HW, cols)
        tv_oth = toth.reshape(n, HW, cols)

        def product(ref, plane):
            lhs = jnp.concatenate([ref[i] for i in range(n)], axis=1)
            return dot(lhs, wgu[pl.ds(pl.multiple_of(plane * half, half), half), :])

        acco[...] = product(tv_own, r)
    with scope("gate_up_other"):
        for i in range(n):
            arrived(toth.at[:, i], osem.at[i])
        part = product(tv_oth, 1 - r)
        for t in range(tiles):
            accx[t] = part[:, t * HW : (t + 1) * HW]

    with scope("activation"):
        arrived(ssp, dsem.at[1])

        def swapped(ref):
            return jnp.concatenate(
                [ref[pl.ds(j * n + i, n, stride=slots), :] for i in range(n) for j in range(SLOTS)], axis=0
            )

        model = 2 * half
        scale = lax.rsqrt((sso[...] + swapped(ssp)) * (1.0 / model) + 1e-06)
        up_at = tiles // 2
        for t in range(up_at):
            gate = (acco[:, t * HW : (t + 1) * HW] + swapped(accx.at[t])) * scale
            up = (acco[:, (t + up_at) * HW : (t + up_at + 1) * HW] + swapped(accx.at[t + up_at])) * scale
            act = gate / (1.0 + jnp.exp(-gate)) * up
            acto[:, t * HW : (t + 1) * HW] = act.astype(BF)
            scr[t] = act
        for t in range(up_at):
            acts[:, t * HW : (t + 1) * HW] = swapped(scr.at[t]).astype(BF)
        remote(acts, actx, 18, dsem.at[2], partner).start()
    with scope("activation_wait"):
        local(wd_hbm.at[0, :, pl.ds(0, half)], wdn.at[first_units], lsem.at[13]).wait()
        arrived(wdn.at[last_units], dsem.at[0])
        arrived(actx, dsem.at[2])

    with scope("down"):
        ov = osend.reshape(n, HW, cols)

        def down(i, c):
            at = pl.ds(pl.multiple_of(i * cols, cols), cols)
            lhs = jnp.concatenate([acto[...], actx[...]], axis=1)
            ov[i] = dot(lhs, wdn[:, at]).astype(BF)

            def to(d, cc):
                uu = around(u, d)
                remote(osend.at[i, uu], gbuf.at[i, u], 19, gsem.at[i], own(uu, v)).start()

            each(to)
            gbuf[i, u] = osend[i, u]
            return c

        lax.fori_loop(0, n, down, 0)

    with scope("combine"):
        gv = gbuf.reshape(n, HW, cols)

        def combine(i, c):
            arrived(gbuf.at[i, most], gsem.at[i])
            both = dot(ctb[...], gv[i], ((0,), (0,)))
            csend[i] = (both[:tokens] + both[tokens:]).astype(BF).reshape(n, tok, cols)

            def to(d, cc):
                vv = around(v, d)
                remote(csend.at[i, vv, mine], zbuf.at[i, 0, v], 20, zsem.at[i, 0], own(u, vv)).start()
                remote(csend.at[i, vv, pl.ds((1 - r) * seqs, seqs)], zbuf.at[i, 1, v], 21, zsem.at[i, 1], across(u, vv)).start()

            each(to)
            remote(csend.at[i, v, pl.ds((1 - r) * seqs, seqs)], zbuf.at[i, 1, v], 21, zsem.at[i, 1], partner).start()
            local(csend.at[i, v, mine], zbuf.at[i, 0, v], lsem.at[0]).start()
            arrived(zbuf.at[0, 0, 0], lsem.at[0])
            return c

        lax.fori_loop(0, n, combine, 0)
    with scope("home_wait"):
        arrived(hm.at[0, most], hmsem.at[0])
        arrived(hm.at[1], hmsem.at[1])
    with scope("final"):
        def final(i, c):
            arrived(zbuf.at[i, 0, most], zsem.at[i, 0])
            arrived(zbuf.at[i, 1], zsem.at[i, 1])
            for p in (0, 1):
                total = hm[p, i]
                for j in range(n):
                    total = total + zbuf[i, p, j].astype(F32)
                plane = r + p - 2 * r * p
                out_ref[:, columns(plane, i)] = total.astype(BF)
            return c

        lax.fori_loop(0, n, final, 0)

    with scope("drain"):
        for send, ref in enumerate((
            wb.at[most, 0], wb.at[:, 0], res.at[most, 0], res.at[:, 0], wdn.at[last_units], id1.at[most], id2.at[most],
            xs.at[0, :, pl.ds(0, (2 * n - 1) * seqs)], xs.at[most], rbuf.at[most], hall.at[most], ss1.at[most], hm.at[0, most],
            town.at[most], ss2.at[most], town, hm.at[1], sso, acts, gbuf.at[most], zbuf.at[:, 0, most], zbuf.at[:, 1],
        )):
            arrived(ref, ssem.at[send])


def solution(mesh):
    n = math.isqrt(mesh.shape["expert"])

    def on_device(queries, token_keys, token_values, stored_keys, stored_values, kv_len, residual, out_weight, norm_gain,
                  expert_ids, route_weight, w_gate, w_up, w_down):
        seqs, pos, kvw = stored_keys.shape
        heads = queries.shape[1] // HW
        model = residual.shape[1]
        half = model // 2
        cols = half // n
        tok, topk = expert_ids.shape
        hidden = w_gate.shape[2]
        tokens = n * tok
        slots = SLOTS * n
        tiles = 2 * hidden // HW
        wrows = out_weight.shape[0]
        vmem = pltpu.VMEM
        dma = pltpu.SemaphoreType.DMA
        scratch = [
            vmem((heads, seqs, HW), BF), vmem((seqs, kvw), BF), vmem((seqs, kvw), BF),
            vmem((seqs, pos, kvw), BF), vmem((seqs, pos, kvw), BF), pltpu.SMEM((seqs,), jnp.int32),
            vmem((model,), BF), vmem((tok, topk), jnp.int32), vmem((tok, topk), F32),
            vmem((model, 2 * hidden), BF), vmem((2 * hidden, half), BF),
            vmem((n, 2, wrows, cols), BF), vmem((n, 2, seqs, cols), BF),
            vmem((n, n, seqs, HW), BF), vmem((n, n, tokens, HW), BF),
            vmem((n, n, tok, cols), BF), vmem((n, n, tok, cols), BF),
            vmem((n, tok, cols), F32), vmem((tokens, cols), BF), vmem((2, n, seqs, cols), F32),
            vmem((n, tokens, cols), BF), vmem((n, n, slots, cols), BF), vmem((n, n, slots, cols), BF), vmem((n, n, slots, cols), BF),
            vmem((topk, HW), F32), vmem((n, topk, HW), F32), vmem((topk, HW), F32), vmem((n, topk, HW), F32),
            vmem((n, HW, HW), BF), vmem((HW, 2 * tokens), BF),
            vmem((n, HW), F32), vmem((n, n, HW), F32), vmem((n, HW), F32), vmem((n, n, HW), F32),
            vmem((HW, HW), F32), vmem((HW, HW), F32),
            vmem((HW, 2 * hidden), F32), vmem((tiles, HW, HW), F32), vmem((tiles // 2, HW, HW), F32),
            vmem((HW, hidden), BF), vmem((HW, hidden), BF), vmem((HW, hidden), BF),
            vmem((n, n, slots, cols), BF), vmem((n, n, slots, cols), BF),
            vmem((n, n, tok, cols), BF), vmem((n, 2, n, seqs, cols), BF),
            dma((15,)), dma((22,)), dma((2,)), dma((2,)), dma((n,)), dma((n, n // 2)), dma, dma((2,)), dma((n,)), dma((n,)), dma((n,)),
            dma, dma, dma, dma, dma((3,)), dma((n,)), dma((n, 2)),
        ]
        return pl.pallas_call(
            functools.partial(kernel, n),
            out_shape=jax.ShapeDtypeStruct(residual.shape, BF),
            in_specs=[pl.BlockSpec(memory_space=pl.ANY)] * 14,
            out_specs=pl.BlockSpec(memory_space=pltpu.VMEM),
            scratch_shapes=scratch,
            compiler_params=pltpu.CompilerParams(
                collective_id=0, has_side_effects=True, vmem_limit_bytes=60 * 1024 * 1024
            ),
        )(queries, token_keys, token_values, stored_keys, stored_values, kv_len, residual, out_weight, norm_gain,
          expert_ids, route_weight, w_gate, w_up, w_down)

    everyone = ("groups", "expert", "replica")
    in_specs = (
        P(everyone, None), P(everyone, None), P(everyone, None), P(everyone, None, None), P(everyone, None, None),
        P(everyone), P(everyone, None), P(("expert", "replica"), None), P(), P(("groups", "expert"), None),
        P(("groups", "expert"), None), P("expert", None, "replica"), P("expert", None, "replica"), P("expert", "replica", None),
    )
    return jax.shard_map(
        on_device, mesh=mesh, in_specs=in_specs, out_specs=P(everyone, None), check_vma=False
    )
```

```python
import functools
import math

import jax
import jax.numpy as jnp
from jax import lax
from jax.experimental import pallas as pl
from jax.experimental.pallas import tpu as pltpu
from jax.sharding import PartitionSpec as P

HW = 128
SLOTS = 2
BF = jnp.bfloat16
F32 = jnp.float32
NEG = -jnp.inf


def dot(a, b, dims=((1,), (0,)), precision=None):
    return lax.dot_general(a, b, (dims, ((), ())), preferred_element_type=F32, precision=precision)


def iota(shape, dim):
    return lax.broadcasted_iota(jnp.int32, shape, dim)


def kernel(
    n, q_hbm, tk_hbm, tv_hbm, k_hbm, v_hbm, len_hbm, res_hbm, ow_hbm, gain_hbm, ids_hbm, rw_hbm, wg_hbm, wu_hbm, wd_hbm,
    out_ref,
    q_s, tk_s, tv_s, k_s, v_s, len_s, gain_s, ids_s, rw_s, wgu, wdn,
    wb, wst, res, att, xs, ysend, rbuf, hid, hg, hm, hall, tsend, town, toth,
    idt, id1, idg, id2, pbuf, ctb, ss0, ss1, ss2t, ss2, sso, ssp,
    acco, accx, scr, acto, acts, actx, osend, gbuf, csend, zbuf,
    lsem, ssem, wsem, rsem, t1sem, xsem, rrsem, hmsem, hsem, tsem, osem, ss1sem, ss2sem, id1sem, id2sem, dsem, gsem, zsem, ready,
):
    r = lax.axis_index("replica")
    e = lax.axis_index("expert")
    x, y = e // n, e % n
    u, v = x * (1 - r) + y * r, y * (1 - r) + x * r
    a, b = n - r * (n - 1), 1 + r * (n - 1)
    heads = n * n
    cols = wb.shape[3]
    half = n * cols
    seqs, pos = k_s.shape[0], k_s.shape[1]
    tok, topk = ids_s.shape
    tokens = n * tok
    slots = SLOTS * n
    most = pl.ds(0, n - 1)
    mesh_id = pl.DeviceIdType.MESH

    def own(uu, vv):
        return {"expert": uu * a + vv * b, "replica": r}

    def across(uu, vv):
        return {"expert": uu * a + vv * b, "replica": 1 - r}

    partner = {"expert": e, "replica": 1 - r}

    def remote(src, dst, send, recv, device):
        return pltpu.make_async_remote_copy(src, dst, ssem.at[send], recv, device_id=device, device_id_type=mesh_id)

    def local(src, dst, sem):
        return pltpu.make_async_copy(src, dst, sem)

    def arrived(ref, sem):
        local(ref, ref, sem).wait()

    def around(w, d):
        return lax.rem(w + d, n)

    def far(i):
        return n // 2 + (2 * lax.rem(i, 2) - 1) * (i // 2)

    def each(body):
        def step(i, c):
            body(far(i), c)
            return c

        lax.fori_loop(1, n, step, 0)

    def columns(plane, block):
        return pl.ds(pl.multiple_of(plane * half + block * cols, cols), cols)

    scope = jax.named_scope

    units = wg_hbm.shape[2]
    first_units, last_units = pl.ds(0, units), pl.ds(units, units)
    with scope("loads"):
        local(k_hbm, k_s, lsem.at[6]).start()

        def qcopy(h, c):
            local(q_hbm.at[:, pl.ds(pl.multiple_of(h * HW, HW), HW)], q_s.at[h], lsem.at[0]).start()
            return c

        lax.fori_loop(0, heads, qcopy, 0)
        local(len_hbm, len_s, lsem.at[1]).start()
        local(tk_hbm, tk_s, lsem.at[2]).start()
        local(tv_hbm, tv_s, lsem.at[3]).start()
        local(v_hbm, v_s, lsem.at[7]).start()
        local(ids_hbm, ids_s, lsem.at[4]).start()
        local(rw_hbm, rw_s, lsem.at[5]).start()

    with scope("barrier"):
        bar = pltpu.get_barrier_semaphore()

        def peers(sem):
            def to(d, c):
                pl.semaphore_signal(sem, device_id={"expert": around(x, d) * n + y, "replica": 1}, device_id_type=mesh_id)
                pl.semaphore_signal(sem, device_id={"expert": x * n + around(y, d), "replica": 1}, device_id_type=mesh_id)
                return c

            lax.fori_loop(1, n, to, 0)

        @pl.when(r == 1)
        def _():
            peers(bar)

        pl.semaphore_wait(bar, r * 2 * (n - 1) + (1 - r))

        @pl.when(r == 1)
        def _():
            pl.semaphore_signal(bar, device_id=partner, device_id_type=mesh_id)

        @pl.when(r == 0)
        def _():
            pl.semaphore_signal(ready.at[0], device_id=partner, device_id_type=mesh_id)

    with scope("weights_send"):

        def wsend(d, c):
            xx, yy = around(x, d), around(y, d)
            remote(ow_hbm.at[:, columns(0, yy)], wst.at[y, r], 0, wsem.at[0, r], {"expert": x * n + yy, "replica": 1}).start()
            remote(ow_hbm.at[:, columns(1, xx)], wb.at[x, r], 1, wsem.at[1, r], {"expert": xx * n + y, "replica": 1}).start()

        each(wsend)

        @pl.when(r == 1)
        def _():
            local(ow_hbm.at[:, columns(0, y)], wst.at[y, r], lsem.at[9]).start()
            local(ow_hbm.at[:, columns(1, x)], wb.at[x, r], lsem.at[9]).start()

        @pl.when(r == 0)
        def _():
            remote(ow_hbm.at[:, columns(0, y)], wst.at[y, r], 2, wsem.at[0, 2], partner).start()
            remote(ow_hbm.at[:, columns(1, x)], wb.at[x, r], 3, wsem.at[1, 2], partner).start()

        local(res_hbm.at[:, columns(r, v)], res.at[v, r], lsem.at[10]).start()
        local(gain_hbm, gain_s, lsem.at[8]).start()
        local(wg_hbm.at[0], wgu.at[:, first_units], lsem.at[11]).start()
        local(wu_hbm.at[0], wgu.at[:, last_units], lsem.at[12]).start()
        local(wd_hbm.at[0, :, pl.ds(pl.multiple_of(r * half, half), half)], wdn.at[first_units], lsem.at[13]).start()

    with scope("attention"):
        kvh = k_s.shape[2] // HW
        per = heads // kvh
        rows = per * seqs
        arrived(q_s, lsem.at[0])
        local(len_hbm, len_s, lsem.at[1]).wait()
        local(tk_hbm, tk_s, lsem.at[2]).wait()
        local(tv_hbm, tv_s, lsem.at[3]).wait()
        local(k_hbm, k_s, lsem.at[6]).wait()
        inv_root = 1.0 / math.sqrt(HW)
        rowseq = lax.rem(iota((rows, pos), 0), seqs)
        colpos = iota((rows, pos), 1)
        visible = jnp.concatenate(
            [jnp.where((rowseq == s) & (colpos < len_s[s]), 0.0, NEG) for s in range(seqs)], axis=1
        )
        fresh_ok = lax.rem(iota((rows, seqs), 0), seqs) == iota((rows, seqs), 1)
        for g in range(kvh):
            at = slice(g * HW, (g + 1) * HW)
            qg = q_s[g * per : (g + 1) * per].reshape(rows, HW)
            kg = k_s[:, :, at].reshape(seqs * pos, HW)
            s_old = dot(qg, kg, ((1,), (1,))) * inv_root + visible
            s_new = jnp.where(fresh_ok, dot(qg, tk_s[:, at], ((1,), (1,))) * inv_root, NEG)
            top = jnp.maximum(jnp.max(s_old, axis=1, keepdims=True), jnp.max(s_new, axis=1, keepdims=True))
            p_old = jnp.exp(s_old - top)
            p_new = jnp.exp(s_new - top)
            scale = 1.0 / (jnp.sum(p_old, axis=1, keepdims=True) + jnp.sum(p_new, axis=1, keepdims=True))
            p_old = (p_old * scale).astype(BF)
            p_new = (p_new * scale).astype(BF).astype(F32)
            if g == 0:
                local(v_hbm, v_s, lsem.at[7]).wait()
            vg = v_s[:, :, at].reshape(seqs * pos, HW)
            mixed = dot(p_old, vg)
            tv = tv_s[:, at].astype(F32)
            for s in range(seqs):
                mixed = mixed + p_new[:, s : s + 1] * tv[s : s + 1, :]
            att[g * (n // kvh) : (g + 1) * (n // kvh)] = mixed.astype(BF).reshape(n // kvh, n, seqs, HW)

    with scope("ids"):
        local(ids_hbm, ids_s, lsem.at[4]).wait()
        local(rw_hbm, rw_s, lsem.at[5]).wait()
        weight = rw_s[...]
        mixing = weight / jnp.sum(weight, axis=1, keepdims=True)
        lane = iota((tok, HW), 1)
        row = iota((tok, HW), 0)
        place = (lane == v * tok + row).astype(F32)
        place_mix = (lane == tokens + v * tok + row).astype(F32)
        exact = lax.Precision.HIGHEST
        idt[...] = dot(ids_s[...].astype(F32), place, ((0,), (0,)), exact) + dot(mixing, place_mix, ((0,), (0,)), exact)
        id1[v] = idt[...]

    with scope("barrier_second"):

        @pl.when(r == 1)
        def _():
            pl.semaphore_wait(ready.at[0], 1)
            peers(ready.at[1])
            pl.semaphore_wait(ready.at[1], 2 * (n - 1))
            pl.semaphore_signal(ready.at[2], device_id=partner, device_id_type=mesh_id)

        @pl.when(r == 0)
        def _():
            pl.semaphore_wait(ready.at[2], 1)

    with scope("feature_send"):
        mine = pl.ds(r * seqs, seqs)

        @pl.when(r == 0)
        def _():
            remote(att.at[:, y], xs.at[x, :, mine], 7, t1sem.at[0], partner).start()

        @pl.when(r == 1)
        def _():
            remote(att.at[x], xs.at[y, :, mine], 7, t1sem.at[0], partner).start()

        def t1send(d, c):
            xx, yy = around(x, d), around(y, d)
            ahead = d // (n // 2)
            place = ahead * (2 * (n - d) - 1) + (1 - ahead) * 2 * d
            rows_at = pl.ds(place * tok + r * seqs, seqs)
            remote(att.at[xx], xs.at[y, :, rows_at], 7, t1sem.at[place], {"expert": xx * n + y, "replica": 0}).start()
            remote(att.at[:, yy], xs.at[x, :, rows_at], 7, t1sem.at[place], {"expert": x * n + yy, "replica": 1}).start()

        each(t1send)

        @pl.when(r == 0)
        def _():
            local(att.at[x], xs.at[y, :, mine], lsem.at[14]).start()

        @pl.when(r == 1)
        def _():
            local(att.at[:, y], xs.at[x, :, mine], lsem.at[14]).start()

        arrived(att.at[0], lsem.at[14])

    with scope("small_send"):

        def idsend(d, c):
            remote(idt, id1.at[v], 5, id1sem, own(u, around(v, d))).start()

        each(idsend)

        def rsend(d, c):
            vv, uu = around(v, d), around(u, d)
            remote(res_hbm.at[:, columns(r, vv)], res.at[v, r], 22, rsem.at[0], own(u, vv)).start()
            remote(res_hbm.at[:, columns(1 - r, uu)], res.at[u, r], 23, rsem.at[1], across(uu, v)).start()

        each(rsend)
        remote(res_hbm.at[:, columns(1 - r, u)], res.at[u, r], 23, rsem.at[1], partner).start()
        remote(wd_hbm.at[0, :, pl.ds(pl.multiple_of((1 - r) * half, half), half)], wdn.at[last_units], 4, dsem.at[0], partner).start()

    chunks = n // 2
    crows = tokens // chunks

    def chunk_of(w, c):
        return xs.at[w, :, pl.ds(c * crows, crows)]

    def pass_on(w, c, d):
        remote(chunk_of(w, c), chunk_of(w, c), 8, xsem.at[w, c], own(u, around(v, d))).start()

    def start_chunk(c):
        for place in (2 * c, 2 * c + 1):
            if place == 0:
                arrived(att.at[0], t1sem.at[0])
            else:
                arrived(att.at[pl.ds(0, 2)], t1sem.at[place])
        for d in (2, n - 2, 1, n - 1):
            pass_on(v, c, d)

    def relay(c):
        behind, ahead = around(v, n - 2), around(v, 2)
        arrived(chunk_of(behind, c), xsem.at[behind, c])
        if c % 2 == 0:
            pass_on(behind, c, 2)
        pass_on(behind, c, 1)
        arrived(chunk_of(ahead, c), xsem.at[ahead, c])
        if c % 2 == 1:
            pass_on(ahead, c, n - 2)
        pass_on(ahead, c, n - 1)

    def gathered(d):
        w = around(v, d)
        for c in range(chunks):
            arrived(chunk_of(w, c), xsem.at[w, c])

    wv = wb.reshape(n * HW, cols)

    def project(blocks):
        lhs = jnp.concatenate(
            [jnp.concatenate([xs[w, k] for k in range(n)], axis=1) for w in blocks], axis=0
        )
        part = dot(lhs, wv[...]).astype(BF)
        for i, w in enumerate(blocks):
            ysend[:, w] = part[i * tokens : (i + 1) * tokens].reshape(n, tok, cols)
            rbuf[u, w] = ysend[0, w]

        def to(d, c):
            uu = around(u, d)
            ahead = d // (n // 2 + 1)
            place = (1 - ahead) * (2 * d - 1) + ahead * 2 * (n - d)
            for w in blocks:
                remote(ysend.at[place, w], rbuf.at[u, w], 9, rrsem, own(uu, v)).start()

        each(to)

    with scope("gather_start"):
        for c in range(chunks):
            start_chunk(c)
    with scope("weights_wait"):

        @pl.when(r == 1)
        def _():
            arrived(wst.at[pl.ds(0, 2), 0], lsem.at[9])
            for p, buf in enumerate((wst, wb)):
                arrived(buf.at[most, 0], wsem.at[p, 0])
                arrived(buf.at[most, 0], wsem.at[p, 1])
                arrived(buf.at[0, 0], wsem.at[p, 2])
            remote(wst, wb, 24, dsem.at[3], partner).start()

    with scope("ids_second"):
        arrived(id1.at[most], id1sem)
        idg[...] = functools.reduce(lambda p, q: p + q, [id1[i] for i in range(n)])

        def id2send(d, c):
            remote(idg, id2.at[u], 6, id2sem, own(around(u, d), v)).start()

        each(id2send)
        id2[u] = idg[...]
    with scope("relay"):
        for c in range(chunks):
            relay(c)
    with scope("weights_wait2"):

        @pl.when(r == 0)
        def _():
            arrived(wb, dsem.at[3])

    with scope("project0"):
        project([v])
    with scope("gather1"):
        gathered(1)
        gathered(n - 1)
    with scope("project1"):
        project([around(v, 1), around(v, n - 1)])
    with scope("project2"):
        project([around(v, 2), around(v, n - 2)])
    with scope("gather3"):
        gathered(3)
        gathered(n - 3)
    with scope("project3"):
        project([around(v, 3), around(v, n - 3)])
    with scope("gather4"):
        gathered(n // 2)
    with scope("project4"):
        project([around(v, n // 2)])

    with scope("tables_wait"):
        arrived(id2.at[most], id2sem)
    with scope("tables"):
        block = (iota((n, HW), 1) // tok == iota((n, HW), 0)).astype(F32)
        before = (
            (iota((HW, HW), 0) // tok == iota((HW, HW), 1) // tok) & (iota((HW, HW), 0) < iota((HW, HW), 1))
        ).astype(BF)
        place_v = iota((n, 1), 0).astype(F32)
        ue = u.astype(F32)
        ve = v.astype(F32)
        ae = a.astype(F32)
        be = b.astype(F32)
        expert_v = ae * ue + be * place_v
        named = []
        for i in range(n):
            got = id2[i]
            named.append(functools.reduce(lambda p, q: p + q, [(got[k : k + 1] == expert_v).astype(F32) for k in range(topk)]))
        named = jnp.concatenate(named, axis=0)
        rank = dot(named.astype(BF), before)
        for i in range(n):
            here = slice(i * n, (i + 1) * n)
            picks = []
            for j in range(SLOTS):
                hit = jnp.where(rank[here] == j, named[here], 0.0)
                picks.append(hit[:, None, :] * block[None])
            pbuf[i] = jnp.stack(picks, axis=1).reshape(HW, HW).astype(BF)
        got = idg[...]
        back = pltpu.roll(got, tokens, 1)
        expert_u = ae * place_v + be * ve
        same = [got[k : k + 1] == expert_u for k in range(topk)]
        chosen = functools.reduce(lambda p, q: p + q, [s.astype(F32) for s in same])
        mix = functools.reduce(lambda p, q: p + q, [jnp.where(s, back[k : k + 1], 0.0) for k, s in enumerate(same)])
        rank = dot(jnp.concatenate([chosen, chosen], axis=0).astype(BF), before)[:n]
        picks = []
        for j in range(SLOTS):
            hit = jnp.where(rank == j, mix, 0.0)
            picks.append(hit[:, None, :] * block[None])
        table = jnp.transpose(jnp.stack(picks, axis=1).reshape(HW, HW))
        high = table.astype(BF).astype(F32)
        low = table - high
        ctb[...] = jnp.concatenate([high[:tokens], low[:tokens]], axis=0).astype(BF)

    with scope("residual_wait"):
        local(res_hbm.at[:, columns(r, v)], res.at[v, r], lsem.at[10]).wait()
        arrived(res.at[most, 0], rsem.at[0])
        arrived(res.at[:, 0], rsem.at[1])
        local(gain_hbm, gain_s, lsem.at[8]).wait()
        gain = gain_s[columns(r, v)].astype(F32).reshape(1, cols)
    with scope("reduce_wait"):
        arrived(rbuf.at[most], rrsem)
    with scope("hidden"):
        total = res[...].astype(F32).reshape(tokens, cols)
        for i in range(n):
            total = total + rbuf[i].astype(F32).reshape(tokens, cols)
        hg[...] = (total * gain).astype(BF)
        hall[u] = hg[...]

        def d1send(i, c):
            d = far(n - i)
            uu = around(u, d)
            remote(hg, hall.at[u], 10, hsem.at[u], own(uu, v)).start()
            return c

        lax.fori_loop(1, n, d1send, 0)
        hid[...] = total.reshape(n, tok, cols)
        square = (total * total).astype(BF)
        sums = dot(jnp.ones((n, cols), BF), square, ((1,), (1,)))
        ss0[...] = jnp.concatenate([sums, jnp.zeros((n, HW - tokens), F32)], axis=1)
        ss1[v] = ss0[...]

        def ss1send(d, c):
            remote(ss0, ss1.at[v], 11, ss1sem, own(u, around(v, d))).start()

        each(ss1send)

    def pack(groups):
        for uu in groups:
            tsend[uu] = dot(pbuf[uu, :, pl.ds(0, tokens)], hall[uu]).astype(BF).reshape(n, slots, cols)

        def to(d, c):
            vv = around(v, d)
            for uu in groups:
                remote(tsend.at[uu, vv], town.at[v, uu], 13, tsem.at[uu], own(u, vv)).start()

        each(to)
        for uu in groups:
            town[v, uu] = tsend[uu, v]

    def pair(s):
        if s == 0:
            return [u]
        if 2 * s == n:
            return [around(u, s)]
        return [around(u, s), around(u, n - s)]

    def pack_pair(s):
        for uu in pair(s):
            if s > 0:
                arrived(hall.at[uu], hsem.at[uu])
        pack(pair(s))

    def hand_over(s):
        for uu in pair(s):
            arrived(town.at[most, uu], tsem.at[uu])
            remote(town.at[:, uu], toth.at[:, uu], 15, osem.at[uu], partner).start()

    with scope("pack0"):
        pack_pair(0)
    with scope("pack1"):
        pack_pair(1)
    with scope("pack2"):
        pack_pair(2)
    with scope("pack3"):
        pack_pair(3)
    with scope("sums_second"):
        arrived(ss1.at[most], ss1sem)
        ss2t[...] = functools.reduce(lambda p, q: p + q, [ss1[i] for i in range(n)])

        def ss2send(d, c):
            remote(ss2t, ss2.at[u], 14, ss2sem, own(around(u, d), v)).start()

        each(ss2send)
        ss2[u] = ss2t[...]
    with scope("pack4"):
        pack_pair(4)
    with scope("hidden_home"):

        def hmsend(d, c):
            vv = around(v, d)
            remote(hid.at[vv, mine], hm.at[0, v], 12, hmsem.at[0], own(u, vv)).start()
            remote(hid.at[vv, pl.ds((1 - r) * seqs, seqs)], hm.at[1, v], 16, hmsem.at[1], across(u, vv)).start()

        each(hmsend)
        remote(hid.at[v, pl.ds((1 - r) * seqs, seqs)], hm.at[1, v], 16, hmsem.at[1], partner).start()
        local(hid.at[v, mine], hm.at[0, v], lsem.at[1]).start()
        arrived(hm.at[0, 0], lsem.at[1])
    with scope("hand0"):
        hand_over(0)
        hand_over(1)
        hand_over(2)
    with scope("expert_weights"):
        local(wg_hbm.at[0], wgu.at[:, first_units], lsem.at[11]).wait()
        local(wu_hbm.at[0], wgu.at[:, last_units], lsem.at[12]).wait()
    with scope("hand3"):
        hand_over(3)
    with scope("hand4"):
        hand_over(4)
    with scope("sums_third"):
        arrived(ss2.at[most], ss2sem)
        for i in range(n):
            part = pbuf[i, pl.ds(pl.multiple_of(v * slots, slots), slots), :].astype(F32)
            column = jnp.sum(part * ss2[i][0:1], axis=1, keepdims=True)
            sso[i * slots : (i + 1) * slots, :] = jnp.broadcast_to(column, (slots, HW))
        remote(sso, ssp, 17, dsem.at[1], partner).start()
    with scope("gate_up_own"):
        tiles = accx.shape[0]
        tv_own = town.reshape(n, HW, cols)
        tv_oth = toth.reshape(n, HW, cols)

        def product(ref, plane):
            lhs = jnp.concatenate([ref[i] for i in range(n)], axis=1)
            return dot(lhs, wgu[pl.ds(pl.multiple_of(plane * half, half), half), :])

        acco[...] = product(tv_own, r)
    with scope("gate_up_other"):
        for i in range(n):
            arrived(toth.at[:, i], osem.at[i])
        part = product(tv_oth, 1 - r)
        for t in range(tiles):
            accx[t] = part[:, t * HW : (t + 1) * HW]

    with scope("activation"):
        arrived(ssp, dsem.at[1])

        def swapped(ref):
            return jnp.concatenate(
                [ref[pl.ds(j * n + i, n, stride=slots), :] for i in range(n) for j in range(SLOTS)], axis=0
            )

        model = 2 * half
        scale = lax.rsqrt((sso[...] + swapped(ssp)) * (1.0 / model) + 1e-06)
        up_at = tiles // 2
        for t in range(up_at):
            gate = (acco[:, t * HW : (t + 1) * HW] + swapped(accx.at[t])) * scale
            up = (acco[:, (t + up_at) * HW : (t + up_at + 1) * HW] + swapped(accx.at[t + up_at])) * scale
            act = gate / (1.0 + jnp.exp(-gate)) * up
            acto[:, t * HW : (t + 1) * HW] = act.astype(BF)
            scr[t] = act
        for t in range(up_at):
            acts[:, t * HW : (t + 1) * HW] = swapped(scr.at[t]).astype(BF)
        remote(acts, actx, 18, dsem.at[2], partner).start()
    with scope("activation_wait"):
        local(wd_hbm.at[0, :, pl.ds(0, half)], wdn.at[first_units], lsem.at[13]).wait()
        arrived(wdn.at[last_units], dsem.at[0])
        arrived(actx, dsem.at[2])

    with scope("down"):
        ov = osend.reshape(n, HW, cols)

        def down(i, c):
            at = pl.ds(pl.multiple_of(i * 2 * cols, 2 * cols), 2 * cols)
            both = dot(jnp.concatenate([acto[...], actx[...]], axis=1), wdn[:, at]).astype(BF)
            for h in (0, 1):
                k = 2 * i + h
                ov[k] = both[:, h * cols : (h + 1) * cols]

                def to(d, cc):
                    uu = around(u, d)
                    remote(osend.at[k, uu], gbuf.at[k, u], 19, gsem.at[k], own(uu, v)).start()

                each(to)
                gbuf[k, u] = osend[k, u]
            return c

        lax.fori_loop(0, n // 2, down, 0)

    with scope("combine"):
        gv = gbuf.reshape(n, HW, cols)

        def combine(i, c):
            arrived(gbuf.at[i, most], gsem.at[i])
            both = dot(ctb[...], gv[i])
            csend[i] = (both[:tokens] + both[tokens:]).astype(BF).reshape(n, tok, cols)

            def to(d, cc):
                vv = around(v, d)
                remote(csend.at[i, vv, mine], zbuf.at[i, 0, v], 20, zsem.at[i, 0], own(u, vv)).start()
                remote(csend.at[i, vv, pl.ds((1 - r) * seqs, seqs)], zbuf.at[i, 1, v], 21, zsem.at[i, 1], across(u, vv)).start()

            each(to)
            remote(csend.at[i, v, pl.ds((1 - r) * seqs, seqs)], zbuf.at[i, 1, v], 21, zsem.at[i, 1], partner).start()
            local(csend.at[i, v, mine], zbuf.at[i, 0, v], lsem.at[0]).start()
            arrived(zbuf.at[0, 0, 0], lsem.at[0])
            return c

        lax.fori_loop(0, n, combine, 0)
    with scope("home_wait"):
        arrived(hm.at[0, most], hmsem.at[0])
        arrived(hm.at[1], hmsem.at[1])
    with scope("final"):
        def final(i, c):
            arrived(zbuf.at[i, 0, most], zsem.at[i, 0])
            arrived(zbuf.at[i, 1], zsem.at[i, 1])
            for p in (0, 1):
                total = hm[p, i]
                for j in range(n):
                    total = total + zbuf[i, p, j].astype(F32)
                plane = r + p - 2 * r * p
                out_ref[:, columns(plane, i)] = total.astype(BF)
            return c

        lax.fori_loop(0, n, final, 0)

    with scope("drain"):
        sent = {
            0: wb.at[most, 0], 1: wb.at[most, 0], 4: wdn.at[last_units], 5: id1.at[most], 6: id2.at[most],
            7: xs.at[0, :, pl.ds(0, (2 * n - 1) * seqs)], 8: xs.at[most], 9: rbuf.at[most], 10: hall.at[most],
            11: ss1.at[most], 12: hm.at[0, most], 13: town.at[most], 14: ss2.at[most], 15: town, 16: hm.at[1], 17: sso,
            18: acts, 19: gbuf.at[most], 20: zbuf.at[:, 0, most], 21: zbuf.at[:, 1], 22: res.at[most, 0], 23: res.at[:, 0],
        }
        for send, ref in sent.items():
            arrived(ref, ssem.at[send])

        @pl.when(r == 0)
        def _():
            arrived(wb.at[0, 0], ssem.at[2])
            arrived(wb.at[0, 0], ssem.at[3])

        @pl.when(r == 1)
        def _():
            arrived(wst, ssem.at[24])


def solution(mesh):
    n = math.isqrt(mesh.shape["expert"])

    def on_device(queries, token_keys, token_values, stored_keys, stored_values, kv_len, residual, out_weight, norm_gain,
                  expert_ids, route_weight, w_gate, w_up, w_down):
        seqs, pos, kvw = stored_keys.shape
        heads = queries.shape[1] // HW
        model = residual.shape[1]
        half = model // 2
        cols = half // n
        tok, topk = expert_ids.shape
        hidden = w_gate.shape[2]
        tokens = n * tok
        slots = SLOTS * n
        tiles = 2 * hidden // HW
        wrows = out_weight.shape[0]
        vmem = pltpu.VMEM
        dma = pltpu.SemaphoreType.DMA
        scratch = [
            vmem((heads, seqs, HW), BF), vmem((seqs, kvw), BF), vmem((seqs, kvw), BF),
            vmem((seqs, pos, kvw), BF), vmem((seqs, pos, kvw), BF), pltpu.SMEM((seqs,), jnp.int32),
            vmem((model,), BF), vmem((tok, topk), jnp.int32), vmem((tok, topk), F32),
            vmem((model, 2 * hidden), BF), vmem((2 * hidden, half), BF),
            vmem((n, 2, wrows, cols), BF), vmem((n, 2, wrows, cols), BF), vmem((n, 2, seqs, cols), BF),
            vmem((n, n, seqs, HW), BF), vmem((n, n, tokens, HW), BF),
            vmem((n, n, tok, cols), BF), vmem((n, n, tok, cols), BF),
            vmem((n, tok, cols), F32), vmem((tokens, cols), BF), vmem((2, n, seqs, cols), F32),
            vmem((n, tokens, cols), BF), vmem((n, n, slots, cols), BF), vmem((n, n, slots, cols), BF), vmem((n, n, slots, cols), BF),
            vmem((topk, HW), F32), vmem((n, topk, HW), F32), vmem((topk, HW), F32), vmem((n, topk, HW), F32),
            vmem((n, HW, HW), BF), vmem((HW, 2 * tokens), BF),
            vmem((n, HW), F32), vmem((n, n, HW), F32), vmem((n, HW), F32), vmem((n, n, HW), F32),
            vmem((HW, HW), F32), vmem((HW, HW), F32),
            vmem((HW, 2 * hidden), F32), vmem((tiles, HW, HW), F32), vmem((tiles // 2, HW, HW), F32),
            vmem((HW, hidden), BF), vmem((HW, hidden), BF), vmem((HW, hidden), BF),
            vmem((n, n, slots, cols), BF), vmem((n, n, slots, cols), BF),
            vmem((n, n, tok, cols), BF), vmem((n, 2, n, seqs, cols), BF),
            dma((15,)), dma((25,)), dma((2, 3)), dma((2,)), dma((n,)), dma((n, n // 2)), dma, dma((2,)), dma((n,)), dma((n,)), dma((n,)),
            dma, dma, dma, dma, dma((4,)), dma((n,)), dma((n, 2)), pltpu.SemaphoreType.REGULAR((3,)),
        ]
        return pl.pallas_call(
            functools.partial(kernel, n),
            out_shape=jax.ShapeDtypeStruct(residual.shape, BF),
            in_specs=[pl.BlockSpec(memory_space=pl.ANY)] * 14,
            out_specs=pl.BlockSpec(memory_space=pltpu.VMEM),
            scratch_shapes=scratch,
            compiler_params=pltpu.CompilerParams(
                collective_id=0, has_side_effects=True, vmem_limit_bytes=60 * 1024 * 1024
            ),
        )(queries, token_keys, token_values, stored_keys, stored_values, kv_len, residual, out_weight, norm_gain,
          expert_ids, route_weight, w_gate, w_up, w_down)

    everyone = ("groups", "expert", "replica")
    in_specs = (
        P(everyone, None), P(everyone, None), P(everyone, None), P(everyone, None, None), P(everyone, None, None),
        P(everyone), P(everyone, None), P(("expert", "replica"), None), P(), P(("groups", "expert"), None),
        P(("groups", "expert"), None), P("expert", None, "replica"), P("expert", None, "replica"), P("expert", "replica", None),
    )
    return jax.shard_map(
        on_device, mesh=mesh, in_specs=in_specs, out_specs=P(everyone, None), check_vma=False
    )
```

```python
import functools
import math

import jax
import jax.numpy as jnp
from jax import lax
from jax.experimental import pallas as pl
from jax.experimental.pallas import tpu as pltpu
from jax.sharding import PartitionSpec as P

HW = 128
SLOTS = 2
BF = jnp.bfloat16
F32 = jnp.float32
NEG = -jnp.inf


def dot(a, b, dims=((1,), (0,)), precision=None):
    return lax.dot_general(a, b, (dims, ((), ())), preferred_element_type=F32, precision=precision)


def iota(shape, dim):
    return lax.broadcasted_iota(jnp.int32, shape, dim)


def kernel(
    n, q_hbm, tk_hbm, tv_hbm, k_hbm, v_hbm, len_hbm, res_hbm, ow_hbm, gain_hbm, ids_hbm, rw_hbm, wg_hbm, wu_hbm, wd_hbm,
    out_ref,
    q_s, tk_s, tv_s, k_s, v_s, len_s, gain_s, ids_s, rw_s, wgu, wdn,
    wb, wst, res, att, xs, ysend, rbuf, hid, hg, hm, hall, tsend, town, toth,
    idt, id1, idg, id2, pbuf, ctb, ss0, ss1, ss2t, ss2, sso, ssp,
    acco, accx, scr, acto, acts, actx, osend, gbuf, csend, zbuf,
    lsem, ssem, wsem, rsem, t1sem, xsem, rrsem, hmsem, hsem, tsem, osem, ss1sem, ss2sem, id1sem, id2sem, dsem, gsem, zsem, ready,
):
    r = lax.axis_index("replica")
    e = lax.axis_index("expert")
    x, y = e // n, e % n
    u, v = x * (1 - r) + y * r, y * (1 - r) + x * r
    a, b = n - r * (n - 1), 1 + r * (n - 1)
    heads = n * n
    cols = wb.shape[3]
    half = n * cols
    seqs, pos = k_s.shape[0], k_s.shape[1]
    tok, topk = ids_s.shape
    tokens = n * tok
    slots = SLOTS * n
    most = pl.ds(0, n - 1)
    mesh_id = pl.DeviceIdType.MESH

    def own(uu, vv):
        return {"expert": uu * a + vv * b, "replica": r}

    def across(uu, vv):
        return {"expert": uu * a + vv * b, "replica": 1 - r}

    partner = {"expert": e, "replica": 1 - r}

    def remote(src, dst, send, recv, device):
        return pltpu.make_async_remote_copy(src, dst, ssem.at[send], recv, device_id=device, device_id_type=mesh_id)

    def local(src, dst, sem):
        return pltpu.make_async_copy(src, dst, sem)

    def arrived(ref, sem):
        local(ref, ref, sem).wait()

    def around(w, d):
        return lax.rem(w + d, n)

    def far(i):
        return n // 2 + (2 * lax.rem(i, 2) - 1) * (i // 2)

    def each(body):
        def step(i, c):
            body(far(i), c)
            return c

        lax.fori_loop(1, n, step, 0)

    def columns(plane, block):
        return pl.ds(pl.multiple_of(plane * half + block * cols, cols), cols)

    scope = jax.named_scope

    units = wg_hbm.shape[2]
    first_units, last_units = pl.ds(0, units), pl.ds(units, units)
    with scope("loads"):
        local(k_hbm, k_s, lsem.at[6]).start()
        local(q_hbm, q_s, lsem.at[0]).start()
        local(len_hbm, len_s, lsem.at[1]).start()
        local(tk_hbm, tk_s, lsem.at[2]).start()
        local(tv_hbm, tv_s, lsem.at[3]).start()
        local(v_hbm, v_s, lsem.at[7]).start()
        local(ids_hbm, ids_s, lsem.at[4]).start()
        local(rw_hbm, rw_s, lsem.at[5]).start()

    with scope("greet"):
        bar = pltpu.get_barrier_semaphore()

        def greet(d, c):
            pl.semaphore_signal(bar, device_id={"expert": around(x, d) * n + y, "replica": r}, device_id_type=mesh_id)
            pl.semaphore_signal(bar, device_id={"expert": x * n + around(y, d), "replica": r}, device_id_type=mesh_id)
            return c

        lax.fori_loop(1, n, greet, 0)

    with scope("attention"):
        kvh = k_s.shape[2] // HW
        per = heads // kvh
        rows = per * seqs
        local(q_hbm, q_s, lsem.at[0]).wait()
        local(len_hbm, len_s, lsem.at[1]).wait()
        local(tk_hbm, tk_s, lsem.at[2]).wait()
        local(tv_hbm, tv_s, lsem.at[3]).wait()
        local(k_hbm, k_s, lsem.at[6]).wait()
        inv_root = 1.0 / math.sqrt(HW)
        rowseq = lax.rem(iota((rows, pos), 0), seqs)
        length = functools.reduce(lambda p, t: jnp.where(rowseq == t, len_s[t], p), range(1, seqs), jnp.full((rows, pos), len_s[0]))
        visible = jnp.where(iota((rows, pos), 1) < length, 0.0, NEG)
        fresh_ok = lax.rem(iota((rows, seqs), 0), seqs) == iota((rows, seqs), 1)

        def of_row(parts):
            mark = rowseq[:, : parts[0].shape[1]]
            return functools.reduce(lambda p, t: jnp.where(mark == t, parts[t], p), range(1, seqs), parts[0])

        for g in range(kvh):
            at = slice(g * HW, (g + 1) * HW)
            qg = jnp.concatenate([q_s[:, (g * per + h) * HW : (g * per + h + 1) * HW] for h in range(per)], axis=0)
            kg = k_s[:, :, at].reshape(seqs * pos, HW)
            every = dot(qg, kg, ((1,), (1,)))
            s_old = of_row([every[:, t * pos : (t + 1) * pos] for t in range(seqs)]) * inv_root + visible
            s_new = dot(qg, tk_s[:, at], ((1,), (1,))) * inv_root
            s_new = jnp.max(jnp.where(fresh_ok, s_new, NEG), axis=1, keepdims=True)
            top = jnp.maximum(jnp.max(s_old, axis=1, keepdims=True), s_new)
            p_old = jnp.exp(s_old - top)
            p_new = jnp.exp(s_new - top)
            scale = 1.0 / (jnp.sum(p_old, axis=1, keepdims=True) + p_new)
            p_old = (p_old * scale).astype(BF)
            p_new = (p_new * scale).astype(BF).astype(F32)
            if g == 0:
                local(v_hbm, v_s, lsem.at[7]).wait()
            every = dot(p_old, jnp.concatenate([v_s[t, :, at] for t in range(seqs)], axis=1))
            mixed = of_row([every[:, t * HW : (t + 1) * HW] for t in range(seqs)])
            tv = tv_s[:, at].astype(F32)
            mixed = mixed + p_new * jnp.concatenate([tv] * per, axis=0)
            att[g * (n // kvh) : (g + 1) * (n // kvh)] = mixed.astype(BF).reshape(n // kvh, n, seqs, HW)

    with scope("entry"):
        pl.semaphore_wait(bar, 2 * (n - 1) + (1 - r))

        @pl.when(r == 1)
        def _():
            pl.semaphore_signal(bar, device_id=partner, device_id_type=mesh_id)

        @pl.when(r == 0)
        def _():
            pl.semaphore_signal(ready.at[0], device_id=partner, device_id_type=mesh_id)

    def weights_send():
        def wsend(d, c):
            xx, yy = around(x, d), around(y, d)
            remote(ow_hbm.at[:, columns(0, yy)], wst.at[y, r], 0, wsem.at[0, r], {"expert": x * n + yy, "replica": 1}).start()
            remote(ow_hbm.at[:, columns(1, xx)], wb.at[x, r], 1, wsem.at[1, r], {"expert": xx * n + y, "replica": 1}).start()

        each(wsend)

    mine = pl.ds(r * seqs, seqs)

    def features_send(plane):
        def t1send(d, c):
            ahead = d // (n // 2)
            place = ahead * (2 * (n - d) - 1) + (1 - ahead) * 2 * d
            rows_at = pl.ds(place * tok + r * seqs, seqs)
            if plane == 0:
                xx = around(x, d)
                remote(att.at[xx], xs.at[y, :, rows_at], 7, t1sem.at[place], {"expert": xx * n + y, "replica": 0}).start()
            else:
                yy = around(y, d)
                remote(att.at[:, yy], xs.at[x, :, rows_at], 7, t1sem.at[place], {"expert": x * n + yy, "replica": 1}).start()

        lax.fori_loop(1, n, lambda i, c: (t1send(far(n - i), c), c)[1], 0)

    with scope("feature_send"):

        @pl.when(r == 0)
        def _():
            features_send(0)
            features_send(1)
            remote(att.at[:, y], xs.at[x, :, mine], 7, t1sem.at[0], partner).start()
            weights_send()
            remote(ow_hbm.at[:, columns(0, y)], wst.at[y, r], 2, wsem.at[0, 2], partner).start()
            remote(ow_hbm.at[:, columns(1, x)], wb.at[x, r], 3, wsem.at[1, 2], partner).start()
            local(att.at[x], xs.at[y, :, mine], lsem.at[14]).start()

        @pl.when(r == 1)
        def _():
            weights_send()
            local(ow_hbm.at[:, columns(0, y)], wst.at[y, r], lsem.at[9]).start()
            local(ow_hbm.at[:, columns(1, x)], wb.at[x, r], lsem.at[9]).start()
            features_send(1)
            local(att.at[:, y], xs.at[x, :, mine], lsem.at[14]).start()
            pl.semaphore_wait(ready.at[0], 1)
            features_send(0)
            remote(att.at[x], xs.at[y, :, mine], 7, t1sem.at[0], partner).start()

        local(res_hbm.at[:, columns(r, v)], res.at[v, r], lsem.at[10]).start()
        local(gain_hbm, gain_s, lsem.at[8]).start()
        arrived(att.at[0], lsem.at[14])

    chunks = n // 2
    crows = tokens // chunks

    def chunk_of(w, c):
        return xs.at[w, :, pl.ds(c * crows, crows)]

    def pass_on(w, c, d):
        remote(chunk_of(w, c), chunk_of(w, c), 8, xsem.at[w, c], own(u, around(v, d))).start()

    def start_chunk(c):
        for place in (2 * c, 2 * c + 1):
            if place == 0:
                arrived(att.at[0], t1sem.at[0])
            else:
                arrived(att.at[pl.ds(0, 2)], t1sem.at[place])
        for d in (2, n - 2, 1, n - 1):
            pass_on(v, c, d)

    def relay(c):
        behind, ahead = around(v, n - 2), around(v, 2)
        arrived(chunk_of(behind, c), xsem.at[behind, c])
        if c % 2 == 0:
            pass_on(behind, c, 2)
        pass_on(behind, c, 1)
        arrived(chunk_of(ahead, c), xsem.at[ahead, c])
        if c % 2 == 1:
            pass_on(ahead, c, n - 2)
        pass_on(ahead, c, n - 1)

    def gathered(d):
        w = around(v, d)
        for c in range(chunks):
            arrived(chunk_of(w, c), xsem.at[w, c])

    wv = wb.reshape(n * HW, cols)

    def project(blocks):
        lhs = jnp.concatenate(
            [jnp.concatenate([xs[w, k] for k in range(n)], axis=1) for w in blocks], axis=0
        )
        part = dot(lhs, wv[...]).astype(BF)
        for i, w in enumerate(blocks):
            ysend[:, w] = part[i * tokens : (i + 1) * tokens].reshape(n, tok, cols)
            rbuf[u, w] = ysend[0, w]

        def to(d, c):
            uu = around(u, d)
            ahead = d // (n // 2 + 1)
            place = (1 - ahead) * (2 * d - 1) + ahead * 2 * (n - d)
            for w in blocks:
                remote(ysend.at[place, w], rbuf.at[u, w], 9, rrsem, own(uu, v)).start()

        each(to)

    with scope("gather_start"):
        start_chunk(0)
        start_chunk(1)

    with scope("ids"):
        local(ids_hbm, ids_s, lsem.at[4]).wait()
        local(rw_hbm, rw_s, lsem.at[5]).wait()
        weight = rw_s[...]
        mixing = weight / jnp.sum(weight, axis=1, keepdims=True)
        lane = iota((tok, HW), 1)
        row = iota((tok, HW), 0)
        place = (lane == v * tok + row).astype(F32)
        place_mix = (lane == tokens + v * tok + row).astype(F32)
        exact = lax.Precision.HIGHEST
        idt[...] = dot(ids_s[...].astype(F32), place, ((0,), (0,)), exact) + dot(mixing, place_mix, ((0,), (0,)), exact)
        id1[v] = idt[...]

        def idsend(d, c):
            remote(idt, id1.at[v], 5, id1sem, own(u, around(v, d))).start()

        each(idsend)

    with scope("gather_third"):
        start_chunk(2)

    with scope("small_send"):

        def rsend(d, c):
            vv, uu = around(v, d), around(u, d)
            remote(res_hbm.at[:, columns(r, vv)], res.at[v, r], 22, rsem.at[0], own(u, vv)).start()
            remote(res_hbm.at[:, columns(1 - r, uu)], res.at[u, r], 23, rsem.at[1], across(uu, v)).start()

        each(rsend)
        remote(res_hbm.at[:, columns(1 - r, u)], res.at[u, r], 23, rsem.at[1], partner).start()

    with scope("gather_last"):
        start_chunk(3)

    with scope("relay"):
        for c in range(chunks // 2):
            relay(c)
    with scope("weights_wait"):

        @pl.when(r == 1)
        def _():
            arrived(wst.at[pl.ds(0, 2), 0], lsem.at[9])
            for p, buf in enumerate((wst, wb)):
                arrived(buf.at[most, 0], wsem.at[p, 0])
                arrived(buf.at[most, 0], wsem.at[p, 1])
                arrived(buf.at[0, 0], wsem.at[p, 2])
            remote(wst, wb, 24, dsem.at[3], partner).start()
    with scope("relay_last"):
        for c in range(chunks // 2, chunks):
            relay(c)
    with scope("expert_loads"):
        local(wg_hbm.at[0], wgu.at[:, first_units], lsem.at[11]).start()
        local(wu_hbm.at[0], wgu.at[:, last_units], lsem.at[12]).start()
        local(wd_hbm.at[0, :, pl.ds(pl.multiple_of(r * half, half), half)], wdn.at[first_units], lsem.at[13]).start()
        remote(wd_hbm.at[0, :, pl.ds(pl.multiple_of((1 - r) * half, half), half)], wdn.at[last_units], 4, dsem.at[0], partner).start()

    with scope("weights_wait2"):

        @pl.when(r == 0)
        def _():
            arrived(wb, dsem.at[3])

    with scope("project0"):
        project([v])
    with scope("gather1"):
        gathered(1)
        gathered(n - 1)
    with scope("project1"):
        project([around(v, 1), around(v, n - 1)])
    with scope("project2"):
        project([around(v, 2), around(v, n - 2)])
    with scope("ids_second"):
        arrived(id1.at[most], id1sem)
        idg[...] = functools.reduce(lambda p, q: p + q, [id1[i] for i in range(n)])

        def id2send(d, c):
            remote(idg, id2.at[u], 6, id2sem, own(around(u, d), v)).start()

        each(id2send)
        id2[u] = idg[...]
    with scope("gather3"):
        gathered(3)
        gathered(n - 3)
    with scope("gather4"):
        gathered(n // 2)
    with scope("project3"):
        project([around(v, 3), around(v, n - 3), around(v, n // 2)])

    with scope("tables_wait"):
        arrived(id2.at[most], id2sem)
    with scope("tables"):
        block = (iota((n, HW), 1) // tok == iota((n, HW), 0)).astype(F32)
        before = (
            (iota((HW, HW), 0) // tok == iota((HW, HW), 1) // tok) & (iota((HW, HW), 0) < iota((HW, HW), 1))
        ).astype(BF)
        place_v = iota((n, 1), 0).astype(F32)
        ue = u.astype(F32)
        ve = v.astype(F32)
        ae = a.astype(F32)
        be = b.astype(F32)
        expert_v = ae * ue + be * place_v
        named = []
        for i in range(n):
            got = id2[i]
            named.append(functools.reduce(lambda p, q: p + q, [(got[k : k + 1] == expert_v).astype(F32) for k in range(topk)]))
        named = jnp.concatenate(named, axis=0)
        rank = dot(named.astype(BF), before)
        for i in range(n):
            here = slice(i * n, (i + 1) * n)
            picks = []
            for j in range(SLOTS):
                hit = jnp.where(rank[here] == j, named[here], 0.0)
                picks.append(hit[:, None, :] * block[None])
            pbuf[i] = jnp.stack(picks, axis=1).reshape(HW, HW).astype(BF)
        got = idg[...]
        back = pltpu.roll(got, tokens, 1)
        expert_u = ae * place_v + be * ve
        same = [got[k : k + 1] == expert_u for k in range(topk)]
        chosen = functools.reduce(lambda p, q: p + q, [s.astype(F32) for s in same])
        mix = functools.reduce(lambda p, q: p + q, [jnp.where(s, back[k : k + 1], 0.0) for k, s in enumerate(same)])
        rank = dot(jnp.concatenate([chosen, chosen], axis=0).astype(BF), before)[:n]
        picks = []
        for j in range(SLOTS):
            hit = jnp.where(rank == j, mix, 0.0)
            picks.append(hit[:, None, :] * block[None])
        table = jnp.transpose(jnp.stack(picks, axis=1).reshape(HW, HW))
        high = table.astype(BF).astype(F32)
        low = table - high
        ctb[...] = jnp.concatenate([high[:tokens], low[:tokens]], axis=0).astype(BF)

    with scope("residual_wait"):
        local(res_hbm.at[:, columns(r, v)], res.at[v, r], lsem.at[10]).wait()
        arrived(res.at[most, 0], rsem.at[0])
        arrived(res.at[:, 0], rsem.at[1])
        local(gain_hbm, gain_s, lsem.at[8]).wait()
        gain = gain_s[columns(r, v)].astype(F32).reshape(1, cols)
    with scope("reduce_wait"):
        arrived(rbuf.at[most], rrsem)
    with scope("hidden"):
        total = res[...].astype(F32).reshape(tokens, cols)
        for i in range(n):
            total = total + rbuf[i].astype(F32).reshape(tokens, cols)
        hg[...] = (total * gain).astype(BF)
        hall[u] = hg[...]

        def d1send(i, c):
            d = far(n - i)
            uu = around(u, d)
            remote(hg, hall.at[u], 10, hsem.at[u], own(uu, v)).start()
            return c

        lax.fori_loop(1, n, d1send, 0)
        hid[...] = total.reshape(n, tok, cols)
        square = (total * total).astype(BF)
        sums = dot(jnp.ones((n, cols), BF), square, ((1,), (1,)))
        ss0[...] = jnp.concatenate([sums, jnp.zeros((n, HW - tokens), F32)], axis=1)
        ss1[v] = ss0[...]

        def ss1send(d, c):
            remote(ss0, ss1.at[v], 11, ss1sem, own(u, around(v, d))).start()

        each(ss1send)

    def pack(groups):
        for uu in groups:
            tsend[uu] = dot(pbuf[uu, :, pl.ds(0, tokens)], hall[uu]).astype(BF).reshape(n, slots, cols)

        def to(d, c):
            vv = around(v, d)
            for uu in groups:
                remote(tsend.at[uu, vv], town.at[v, uu], 13, tsem.at[uu], own(u, vv)).start()

        each(to)
        for uu in groups:
            town[v, uu] = tsend[uu, v]

    def pair(s):
        if s == 0:
            return [u]
        if 2 * s == n:
            return [around(u, s)]
        return [around(u, s), around(u, n - s)]

    def pack_pair(s):
        for uu in pair(s):
            if s > 0:
                arrived(hall.at[uu], hsem.at[uu])
        pack(pair(s))

    def hand_over(s):
        for uu in pair(s):
            arrived(town.at[most, uu], tsem.at[uu])
            remote(town.at[:, uu], toth.at[:, uu], 15, osem.at[uu], partner).start()

    with scope("pack0"):
        pack_pair(0)
    with scope("pack1"):
        pack_pair(1)
    with scope("pack2"):
        pack_pair(2)
    with scope("pack3"):
        pack_pair(3)
    with scope("sums_second"):
        arrived(ss1.at[most], ss1sem)
        ss2t[...] = functools.reduce(lambda p, q: p + q, [ss1[i] for i in range(n)])

        def ss2send(d, c):
            remote(ss2t, ss2.at[u], 14, ss2sem, own(around(u, d), v)).start()

        each(ss2send)
        ss2[u] = ss2t[...]
    with scope("pack4"):
        pack_pair(4)
    with scope("hand0"):
        hand_over(0)
        hand_over(1)
        hand_over(2)
    with scope("expert_weights"):
        local(wg_hbm.at[0], wgu.at[:, first_units], lsem.at[11]).wait()
        local(wu_hbm.at[0], wgu.at[:, last_units], lsem.at[12]).wait()
    with scope("hand3"):
        hand_over(3)
    with scope("hand4"):
        hand_over(4)
    with scope("sums_third"):
        arrived(ss2.at[most], ss2sem)
        for i in range(n):
            part = pbuf[i, pl.ds(pl.multiple_of(v * slots, slots), slots), :].astype(F32)
            column = jnp.sum(part * ss2[i][0:1], axis=1, keepdims=True)
            sso[i * slots : (i + 1) * slots, :] = jnp.broadcast_to(column, (slots, HW))
        remote(sso, ssp, 17, dsem.at[1], partner).start()
    with scope("gate_up_own"):
        tiles = accx.shape[0]
        tv_own = town.reshape(n, HW, cols)
        tv_oth = toth.reshape(n, HW, cols)

        def product(ref, plane):
            lhs = jnp.concatenate([ref[i] for i in range(n)], axis=1)
            return dot(lhs, wgu[pl.ds(pl.multiple_of(plane * half, half), half), :])

        acco[...] = product(tv_own, r)
    with scope("gate_up_other"):
        for i in range(n):
            arrived(toth.at[:, i], osem.at[i])
        part = product(tv_oth, 1 - r)
        for t in range(tiles):
            accx[t] = part[:, t * HW : (t + 1) * HW]

    with scope("activation"):
        arrived(ssp, dsem.at[1])

        def swapped(ref):
            return jnp.concatenate(
                [ref[pl.ds(j * n + i, n, stride=slots), :] for i in range(n) for j in range(SLOTS)], axis=0
            )

        model = 2 * half
        scale = lax.rsqrt((sso[...] + swapped(ssp)) * (1.0 / model) + 1e-06)
        up_at = tiles // 2
        for t in range(up_at):
            gate = (acco[:, t * HW : (t + 1) * HW] + swapped(accx.at[t])) * scale
            up = (acco[:, (t + up_at) * HW : (t + up_at + 1) * HW] + swapped(accx.at[t + up_at])) * scale
            act = gate / (1.0 + jnp.exp(-gate)) * up
            acto[:, t * HW : (t + 1) * HW] = act.astype(BF)
            scr[t] = act
        for t in range(up_at):
            acts[:, t * HW : (t + 1) * HW] = swapped(scr.at[t]).astype(BF)
        remote(acts, actx, 18, dsem.at[2], partner).start()
    with scope("hidden_home"):

        def hmsend(d, c):
            vv = around(v, d)
            remote(hid.at[vv, mine], hm.at[0, v], 12, hmsem.at[0], own(u, vv)).start()
            remote(hid.at[vv, pl.ds((1 - r) * seqs, seqs)], hm.at[1, v], 16, hmsem.at[1], across(u, vv)).start()

        each(hmsend)
        remote(hid.at[v, pl.ds((1 - r) * seqs, seqs)], hm.at[1, v], 16, hmsem.at[1], partner).start()
        local(hid.at[v, mine], hm.at[0, v], lsem.at[1]).start()
        arrived(hm.at[0, 0], lsem.at[1])
    with scope("activation_wait"):
        local(wd_hbm.at[0, :, pl.ds(0, half)], wdn.at[first_units], lsem.at[13]).wait()
        arrived(wdn.at[last_units], dsem.at[0])
        arrived(actx, dsem.at[2])

    with scope("down"):
        ov = osend.reshape(n, HW, cols)

        def down(first, count):
            at = slice(first * cols, (first + count) * cols)
            part = dot(jnp.concatenate([acto[...], actx[...]], axis=1), wdn[:, at]).astype(BF)
            for h in range(count):
                k = first + h
                ov[k] = part[:, h * cols : (h + 1) * cols]

                def to(d, c):
                    uu = around(u, d)
                    remote(osend.at[k, uu], gbuf.at[k, u], 19, gsem.at[k], own(uu, v)).start()

                each(to)
                gbuf[k, u] = osend[k, u]

        down(0, 1)
        down(1, 1)
        for first in range(2, n, 2):
            down(first, 2)

    with scope("combine"):
        gv = gbuf.reshape(n, HW, cols)

        def combine(i, c):
            arrived(gbuf.at[i, most], gsem.at[i])
            both = dot(ctb[...], gv[i])
            csend[i] = (both[:tokens] + both[tokens:]).astype(BF).reshape(n, tok, cols)

            def to(d, cc):
                vv = around(v, d)
                remote(csend.at[i, vv, mine], zbuf.at[i, 0, v], 20, zsem.at[i, 0], own(u, vv)).start()
                remote(csend.at[i, vv, pl.ds((1 - r) * seqs, seqs)], zbuf.at[i, 1, v], 21, zsem.at[i, 1], across(u, vv)).start()

            each(to)
            remote(csend.at[i, v, pl.ds((1 - r) * seqs, seqs)], zbuf.at[i, 1, v], 21, zsem.at[i, 1], partner).start()
            local(csend.at[i, v, mine], zbuf.at[i, 0, v], lsem.at[0]).start()
            arrived(zbuf.at[0, 0, 0], lsem.at[0])
            return c

        lax.fori_loop(0, n, combine, 0)
    with scope("home_wait"):
        arrived(hm.at[0, most], hmsem.at[0])
        arrived(hm.at[1], hmsem.at[1])
    with scope("final"):
        def final(i, c):
            arrived(zbuf.at[i, 0, most], zsem.at[i, 0])
            arrived(zbuf.at[i, 1], zsem.at[i, 1])
            for p in (0, 1):
                total = hm[p, i]
                for j in range(n):
                    total = total + zbuf[i, p, j].astype(F32)
                plane = r + p - 2 * r * p
                out_ref[:, columns(plane, i)] = total.astype(BF)
            return c

        lax.fori_loop(0, n, final, 0)

    with scope("drain"):
        sent = {
            0: wb.at[most, 0], 1: wb.at[most, 0], 4: wdn.at[last_units], 5: id1.at[most], 6: id2.at[most],
            7: xs.at[0, :, pl.ds(0, (2 * n - 1) * seqs)], 8: xs.at[most], 9: rbuf.at[most], 10: hall.at[most],
            11: ss1.at[most], 12: hm.at[0, most], 13: town.at[most], 14: ss2.at[most], 15: town, 16: hm.at[1], 17: sso,
            18: acts, 19: gbuf.at[most], 20: zbuf.at[:, 0, most], 21: zbuf.at[:, 1], 22: res.at[most, 0], 23: res.at[:, 0],
        }
        for send, ref in sent.items():
            arrived(ref, ssem.at[send])

        @pl.when(r == 0)
        def _():
            arrived(wb.at[0, 0], ssem.at[2])
            arrived(wb.at[0, 0], ssem.at[3])

        @pl.when(r == 1)
        def _():
            arrived(wst, ssem.at[24])


def solution(mesh):
    n = math.isqrt(mesh.shape["expert"])

    def on_device(queries, token_keys, token_values, stored_keys, stored_values, kv_len, residual, out_weight, norm_gain,
                  expert_ids, route_weight, w_gate, w_up, w_down):
        seqs, pos, kvw = stored_keys.shape
        heads = queries.shape[1] // HW
        model = residual.shape[1]
        half = model // 2
        cols = half // n
        tok, topk = expert_ids.shape
        hidden = w_gate.shape[2]
        tokens = n * tok
        slots = SLOTS * n
        tiles = 2 * hidden // HW
        wrows = out_weight.shape[0]
        vmem = pltpu.VMEM
        dma = pltpu.SemaphoreType.DMA
        scratch = [
            vmem((seqs, heads * HW), BF), vmem((seqs, kvw), BF), vmem((seqs, kvw), BF),
            vmem((seqs, pos, kvw), BF), vmem((seqs, pos, kvw), BF), pltpu.SMEM((seqs,), jnp.int32),
            vmem((model,), BF), vmem((tok, topk), jnp.int32), vmem((tok, topk), F32),
            vmem((model, 2 * hidden), BF), vmem((2 * hidden, half), BF),
            vmem((n, 2, wrows, cols), BF), vmem((n, 2, wrows, cols), BF), vmem((n, 2, seqs, cols), BF),
            vmem((n, n, seqs, HW), BF), vmem((n, n, tokens, HW), BF),
            vmem((n, n, tok, cols), BF), vmem((n, n, tok, cols), BF),
            vmem((n, tok, cols), F32), vmem((tokens, cols), BF), vmem((2, n, seqs, cols), F32),
            vmem((n, tokens, cols), BF), vmem((n, n, slots, cols), BF), vmem((n, n, slots, cols), BF), vmem((n, n, slots, cols), BF),
            vmem((topk, HW), F32), vmem((n, topk, HW), F32), vmem((topk, HW), F32), vmem((n, topk, HW), F32),
            vmem((n, HW, HW), BF), vmem((HW, 2 * tokens), BF),
            vmem((n, HW), F32), vmem((n, n, HW), F32), vmem((n, HW), F32), vmem((n, n, HW), F32),
            vmem((HW, HW), F32), vmem((HW, HW), F32),
            vmem((HW, 2 * hidden), F32), vmem((tiles, HW, HW), F32), vmem((tiles // 2, HW, HW), F32),
            vmem((HW, hidden), BF), vmem((HW, hidden), BF), vmem((HW, hidden), BF),
            vmem((n, n, slots, cols), BF), vmem((n, n, slots, cols), BF),
            vmem((n, n, tok, cols), BF), vmem((n, 2, n, seqs, cols), BF),
            dma((15,)), dma((25,)), dma((2, 3)), dma((2,)), dma((n,)), dma((n, n // 2)), dma, dma((2,)), dma((n,)), dma((n,)), dma((n,)),
            dma, dma, dma, dma, dma((4,)), dma((n,)), dma((n, 2)), pltpu.SemaphoreType.REGULAR((1,)),
        ]
        return pl.pallas_call(
            functools.partial(kernel, n),
            out_shape=pltpu.VMEM(residual.shape, BF),
            in_specs=[pl.BlockSpec(memory_space=pl.ANY)] * 14,
            out_specs=pl.BlockSpec(memory_space=pltpu.VMEM),
            scratch_shapes=scratch,
            compiler_params=pltpu.CompilerParams(
                collective_id=0, has_side_effects=True, vmem_limit_bytes=60 * 1024 * 1024
            ),
        )(queries, token_keys, token_values, stored_keys, stored_values, kv_len, residual, out_weight, norm_gain,
          expert_ids, route_weight, w_gate, w_up, w_down)

    everyone = ("groups", "expert", "replica")
    in_specs = (
        P(everyone, None), P(everyone, None), P(everyone, None), P(everyone, None, None), P(everyone, None, None),
        P(everyone), P(everyone, None), P(("expert", "replica"), None), P(), P(("groups", "expert"), None),
        P(("groups", "expert"), None), P("expert", None, "replica"), P("expert", None, "replica"), P("expert", "replica", None),
    )
    return jax.shard_map(
        on_device, mesh=mesh, in_specs=in_specs, out_specs=P(everyone, None), check_vma=False
    )
```
